8 devices in a mesh: dp: 2 (over z, y), tp: 4 (over x, core).
Axes of the slice: x: 2, y: 2, z: 1, core: 2. Of those that a mesh axis runs over, the one named last changes fastest.
Arguments:
- hidden: bfloat16 [2, 64, 4096], P('dp', 'tp'), parts along dimension 0
- vision: bfloat16 [2, 256, 4096], P('dp', 'tp'), parts along dimension 0
- positions: int32 [2, 64], P('dp', 'tp'), parts along dimension 0
- tile_mask: int32 [2, 64, 4], P('dp', 'tp'), parts along dimension 0
- ln1_a: bfloat16 [4096], replicated
- wq_a: bfloat16 [4096, 4096], P(None, 'tp')
- wk_a: bfloat16 [4096, 1024], P(None, 'tp')
- wv_a: bfloat16 [4096, 1024], P(None, 'tp')
- wo_a: bfloat16 [4096, 4096], P('tp')
- ln2_a: bfloat16 [4096], replicated
- wg_a: bfloat16 [4096, 14336], P(None, 'tp')
- wu_a: bfloat16 [4096, 14336], P(None, 'tp')
- wd_a: bfloat16 [14336, 4096], P('tp')
- ln1_b: bfloat16 [4096], replicated
- wq_b: bfloat16 [4096, 4096], P(None, 'tp')
- q_norm: bfloat16 [128], replicated
- wk_b: bfloat16 [4096, 1024], P(None, 'tp')
- wv_b: bfloat16 [4096, 1024], P(None, 'tp')
- k_norm: bfloat16 [128], replicated
- wo_b: bfloat16 [4096, 4096], P('tp')
- ln2_b: bfloat16 [4096], replicated
- wg_b: bfloat16 [4096, 14336], P(None, 'tp')
- wu_b: bfloat16 [4096, 14336], P(None, 'tp')
- wd_b: bfloat16 [14336, 4096], P('tp')
- xgates: float32 [2], replicated
Outputs:
- output: bfloat16 [2, 64, 4096], P('dp', 'tp'), parts along dimension 0
There are 2 independent parts. The reference program is written for one: setup_inputs(seed, part) draws one part's arguments, and reference() takes and returns one part's arrays. A program takes and returns all parts, laid end to end along the dimension named above; an argument that names none is the same for every part.
All inputs are finite; a program needn't handle non-finite values.
Results may differ from the reference program's by a relative error of at most 0.0161159.
Values are sent between devices in bfloat16 or wider.
A program may use at most 1 GiB of HBM per device.

```python
import math
import jax
import jax.numpy as jnp
from jax import lax

SAMPLES = 1
TOKENS = 64
VISION_TOKENS = 256
MODEL_DIM = 4096
NUM_HEADS = 32
KV_HEADS = 8
HEAD_DIM = 128
FFN_DIM = 14336
NUM_TILES = 4

ROPE_THETA = 500000.0
ROPE_FACTOR = 8.0
LOW_FACTOR = 1.0
HIGH_FACTOR = 4.0
ORIG_CONTEXT = 8192.0
NORM_EPS = 1e-5
MASK_VALUE = -1e30


def rope_table(head_dim):
    low_wave = ORIG_CONTEXT / LOW_FACTOR
    high_wave = ORIG_CONTEXT / HIGH_FACTOR
    freq_list = []
    for freq_idx in range(head_dim // 2):
        base_freq = 1.0 / (ROPE_THETA ** (2.0 * freq_idx / head_dim))
        wave_len = 2.0 * math.pi / base_freq
        if wave_len > low_wave:
            freq_list.append(base_freq / ROPE_FACTOR)
        elif wave_len < high_wave:
            freq_list.append(base_freq)
        else:
            smooth = (ORIG_CONTEXT / wave_len - LOW_FACTOR) / (HIGH_FACTOR - LOW_FACTOR)
            freq_list.append((1.0 - smooth) * base_freq / ROPE_FACTOR + smooth * base_freq)
    return jnp.array(freq_list, dtype=jnp.float32)


def rms_scale(values, norm_gain):
    values = values.astype(jnp.float32)
    mean_sq = jnp.mean(values * values, axis=-1, keepdims=True)
    return values * lax.rsqrt(mean_sq + NORM_EPS) * norm_gain.astype(jnp.float32)


def rotate(values, cos_tab, sin_tab):
    half_dim = values.shape[-1] // 2
    first_half = values[..., :half_dim]
    second_half = values[..., half_dim:]
    return jnp.concatenate([first_half * cos_tab - second_half * sin_tab, second_half * cos_tab + first_half * sin_tab], axis=-1)


def group_attention(queries, key_vecs, val_vecs, allowed):
    def one_group(operands):
        query_grp, key_grp, val_grp = operands
        scores = jnp.einsum('rqd,kd->rqk', query_grp.astype(jnp.float32), key_grp.astype(jnp.float32)) * (HEAD_DIM ** -0.5)
        weights = jax.nn.softmax(jnp.where(allowed[None], scores, MASK_VALUE), axis=-1).astype(jnp.bfloat16)
        return jnp.einsum('rqk,kd->rqd', weights.astype(jnp.float32), val_grp.astype(jnp.float32)).astype(jnp.bfloat16)
    grouped = lax.map(one_group, (jnp.transpose(queries, (1, 2, 0, 3)), jnp.transpose(key_vecs, (1, 0, 2)), jnp.transpose(val_vecs, (1, 0, 2))))
    return jnp.transpose(grouped, (2, 0, 1, 3)).reshape(queries.shape[0], -1)


def gated_mlp(resid, norm_gain, w_gate, w_up, w_down):
    normed = rms_scale(resid, norm_gain).astype(jnp.bfloat16)
    gate_proj = jnp.dot(normed, w_gate, preferred_element_type=jnp.float32)
    up_proj = jnp.dot(normed, w_up, preferred_element_type=jnp.float32)
    activated = (jax.nn.silu(gate_proj) * up_proj).astype(jnp.bfloat16)
    return jnp.dot(activated, w_down, preferred_element_type=jnp.float32)


def setup_inputs(seed: int = 0, part: int = 0) -> dict:
    data_keys = jax.random.split(jax.random.fold_in(jax.random.key(seed + 1), part), 6)
    weight_keys = jax.random.split(jax.random.key(seed), 22)
    qk_scale = max(math.log(TOKENS / 8.0), 1.0) ** 0.25
    cross_gain = max(math.log(VISION_TOKENS / 16.0), 1.0) ** 0.25
    q_width = NUM_HEADS * HEAD_DIM
    kv_width = KV_HEADS * HEAD_DIM
    dim_scale = MODEL_DIM ** -0.5

    def draw_normal(key_val, arr_shape, spread):
        return (jax.random.normal(key_val, arr_shape, jnp.float32) * spread).astype(jnp.bfloat16)

    def draw_gain(key_val, arr_shape, center):
        return (center * (1.0 + 0.2 * jax.random.normal(key_val, arr_shape, jnp.float32))).astype(jnp.bfloat16)

    hidden = draw_normal(data_keys[0], (SAMPLES, TOKENS, MODEL_DIM), 1.0)
    vision = draw_normal(data_keys[1], (SAMPLES, VISION_TOKENS, MODEL_DIM), 1.0)
    pos_steps = jax.random.randint(data_keys[2], (SAMPLES, TOKENS), 1, 4, dtype=jnp.int32)
    offsets = jax.random.randint(data_keys[3], (SAMPLES, 1), 0, TOKENS, dtype=jnp.int32)
    positions = (offsets + jnp.cumsum(pos_steps, axis=1)).astype(jnp.int32)
    begins = jax.random.randint(data_keys[4], (SAMPLES, 1, 1), 0, TOKENS // 4 + 1, dtype=jnp.int32)
    tile_bits = jax.random.randint(data_keys[5], (SAMPLES, TOKENS, NUM_TILES), 0, 2, dtype=jnp.int32)
    tile_mask = jnp.where(jnp.arange(TOKENS, dtype=jnp.int32)[None, :, None] >= begins, tile_bits, 0).astype(jnp.int32)
    magnitudes = jax.random.uniform(weight_keys[20], (2,), jnp.float32, 0.6, 1.4)
    gate_signs = (2 * jax.random.randint(weight_keys[21], (2,), 0, 2, dtype=jnp.int32) - 1).astype(jnp.float32)
    return {
        'hidden': hidden,
        'vision': vision,
        'positions': positions,
        'tile_mask': tile_mask,
        'ln1_a': draw_gain(weight_keys[0], (MODEL_DIM,), 1.0),
        'wq_a': draw_normal(weight_keys[1], (MODEL_DIM, q_width), qk_scale * dim_scale),
        'wk_a': draw_normal(weight_keys[2], (MODEL_DIM, kv_width), qk_scale * dim_scale),
        'wv_a': draw_normal(weight_keys[3], (MODEL_DIM, kv_width), dim_scale),
        'wo_a': draw_normal(weight_keys[4], (q_width, MODEL_DIM), q_width ** -0.5),
        'ln2_a': draw_gain(weight_keys[5], (MODEL_DIM,), 1.0),
        'wg_a': draw_normal(weight_keys[6], (MODEL_DIM, FFN_DIM), dim_scale),
        'wu_a': draw_normal(weight_keys[7], (MODEL_DIM, FFN_DIM), dim_scale),
        'wd_a': draw_normal(weight_keys[8], (FFN_DIM, MODEL_DIM), FFN_DIM ** -0.5),
        'ln1_b': draw_gain(weight_keys[9], (MODEL_DIM,), 1.0),
        'wq_b': draw_normal(weight_keys[10], (MODEL_DIM, q_width), dim_scale),
        'q_norm': draw_gain(weight_keys[11], (HEAD_DIM,), cross_gain),
        'wk_b': draw_normal(weight_keys[12], (MODEL_DIM, kv_width), dim_scale),
        'wv_b': draw_normal(weight_keys[13], (MODEL_DIM, kv_width), dim_scale),
        'k_norm': draw_gain(weight_keys[14], (HEAD_DIM,), cross_gain),
        'wo_b': draw_normal(weight_keys[15], (q_width, MODEL_DIM), q_width ** -0.5),
        'ln2_b': draw_gain(weight_keys[16], (MODEL_DIM,), 1.0),
        'wg_b': draw_normal(weight_keys[17], (MODEL_DIM, FFN_DIM), dim_scale),
        'wu_b': draw_normal(weight_keys[18], (MODEL_DIM, FFN_DIM), dim_scale),
        'wd_b': draw_normal(weight_keys[19], (FFN_DIM, MODEL_DIM), FFN_DIM ** -0.5),
        'xgates': magnitudes * gate_signs,
    }


def reference(hidden, vision, positions, tile_mask, ln1_a, wq_a, wk_a, wv_a, wo_a, ln2_a, wg_a, wu_a, wd_a, ln1_b, wq_b, q_norm, wk_b, wv_b, k_norm, wo_b, ln2_b, wg_b, wu_b, wd_b, xgates):
    rep_heads = NUM_HEADS // KV_HEADS
    tile_len = VISION_TOKENS // NUM_TILES
    inv_freq = rope_table(HEAD_DIM)
    gate_vals = jnp.tanh(xgates.astype(jnp.float32))
    causal = lax.broadcasted_iota(jnp.int32, (TOKENS, TOKENS), 0) >= lax.broadcasted_iota(jnp.int32, (TOKENS, TOKENS), 1)

    def one_sample(operands):
        hid_rows, vis_rows, pos_row, mask_row = operands
        angles = pos_row.astype(jnp.float32)[:, None] * inv_freq[None, :]
        cos_tab = jnp.cos(angles)[:, None, :]
        sin_tab = jnp.sin(angles)[:, None, :]
        normed = rms_scale(hid_rows, ln1_a).astype(jnp.bfloat16)
        queries = jnp.dot(normed, wq_a, preferred_element_type=jnp.float32).reshape(TOKENS, NUM_HEADS, HEAD_DIM)
        queries = rotate(queries, cos_tab, sin_tab).astype(jnp.bfloat16).reshape(TOKENS, KV_HEADS, rep_heads, HEAD_DIM)
        key_vecs = jnp.dot(normed, wk_a, preferred_element_type=jnp.float32).reshape(TOKENS, KV_HEADS, HEAD_DIM)
        key_vecs = rotate(key_vecs, cos_tab, sin_tab).astype(jnp.bfloat16)
        val_vecs = jnp.dot(normed, wv_a, preferred_element_type=jnp.float32).astype(jnp.bfloat16).reshape(TOKENS, KV_HEADS, HEAD_DIM)
        context = group_attention(queries, key_vecs, val_vecs, causal)
        h_one = (hid_rows.astype(jnp.float32) + jnp.dot(context, wo_a, preferred_element_type=jnp.float32)).astype(jnp.bfloat16)
        h_two = (h_one.astype(jnp.float32) + gated_mlp(h_one, ln2_a, wg_a, wu_a, wd_a)).astype(jnp.bfloat16)
        normed = rms_scale(h_two, ln1_b).astype(jnp.bfloat16)
        queries = jnp.dot(normed, wq_b, preferred_element_type=jnp.float32).reshape(TOKENS, NUM_HEADS, HEAD_DIM)
        queries = rms_scale(queries, q_norm).astype(jnp.bfloat16).reshape(TOKENS, KV_HEADS, rep_heads, HEAD_DIM)
        key_vecs = jnp.dot(vis_rows, wk_b, preferred_element_type=jnp.float32).reshape(VISION_TOKENS, KV_HEADS, HEAD_DIM)
        key_vecs = rms_scale(key_vecs, k_norm).astype(jnp.bfloat16)
        val_vecs = jnp.dot(vis_rows, wv_b, preferred_element_type=jnp.float32).astype(jnp.bfloat16).reshape(VISION_TOKENS, KV_HEADS, HEAD_DIM)
        visible = mask_row > 0
        allowed = jnp.repeat(visible, tile_len, axis=1)
        context = group_attention(queries, key_vecs, val_vecs, allowed)
        row_keep = jnp.any(visible, axis=-1, keepdims=True).astype(jnp.float32)
        attn_out = jnp.dot(context, wo_b, preferred_element_type=jnp.float32)
        h_three = (h_two.astype(jnp.float32) + gate_vals[0] * row_keep * attn_out).astype(jnp.bfloat16)
        mlp_out = gated_mlp(h_three, ln2_b, wg_b, wu_b, wd_b)
        return (h_three.astype(jnp.float32) + gate_vals[1] * row_keep * mlp_out).astype(jnp.bfloat16)

    return lax.map(one_sample, (hidden, vision, positions, tile_mask))
```

```python
import math
import jax
import jax.numpy as jnp
import numpy as np
from jax import lax
from jax.experimental import pallas as pl
from jax.experimental.pallas import tpu as pltpu
from jax.sharding import PartitionSpec as P

ROPE_THETA = 500000.0
ROPE_FACTOR = 8.0
LOW_FACTOR = 1.0
HIGH_FACTOR = 4.0
ORIG_CONTEXT = 8192.0
NORM_EPS = 1e-5
MASK_VALUE = -1e30
MESH = pl.DeviceIdType.MESH
BF16 = jnp.bfloat16
F32 = jnp.float32

T = 64
TB = 16
D = 4096
V = 256
VB = 64
HD = 128
KV = 2
REP = 4
FF = 3584
NC = 256
SP = 13
WO_ROWS = KV * REP * HD

SEGMENTS = []
_at = 0
for _name, _count in (('qa', 2), ('kva', 1), ('oa', 2), ('gua', 14), ('da', 8),
                      ('kvb', 1), ('qb', 2), ('ob', 2), ('gub', 14), ('db', 8)):
    SEGMENTS.append((_name, _at, _count))
    _at += _count
TOTAL = _at
BASE = {name: first for name, first, _ in SEGMENTS}


def rope_table(head_dim):
    low_wave = ORIG_CONTEXT / LOW_FACTOR
    high_wave = ORIG_CONTEXT / HIGH_FACTOR
    freq_list = []
    for freq_idx in range(head_dim // 2):
        base_freq = 1.0 / (ROPE_THETA ** (2.0 * freq_idx / head_dim))
        wave_len = 2.0 * math.pi / base_freq
        if wave_len > low_wave:
            freq_list.append(base_freq / ROPE_FACTOR)
        elif wave_len < high_wave:
            freq_list.append(base_freq)
        else:
            smooth = (ORIG_CONTEXT / wave_len - LOW_FACTOR) / (HIGH_FACTOR - LOW_FACTOR)
            freq_list.append((1.0 - smooth) * base_freq / ROPE_FACTOR + smooth * base_freq)
    return np.array(freq_list, dtype=np.float32)


def dot(a, b):
    return jnp.dot(a, b, preferred_element_type=F32)


def dot_t(a, b):
    return lax.dot_general(a, b, (((1,), (1,)), ((), ())), preferred_element_type=F32)


def kernel(hid, vis, pos, tmask, freq,
           ln1a, wqa, wka, wva, woa, ln2a, wga, wua, wda,
           ln1b, wqb, qn, wkb, wvb, kn, wob, ln2b, wgb, wub, wdb, xg,
           out,
           wbuf, wsem, hx, posb, maskb, cosb, sinb, h, x, act, ctx, qb, kb, vb, vg,
           pb, rcv1, snd2, rcv2, pf, rcvf,
           lsem, hs, hr, ps, pr, ms, mr, vs, vr, s1, r1, s2, r2, s3, r3, fs, fr):
    d = lax.axis_index('tp')
    core = lax.rem(d, 2)
    part = d + 1 - 2 * core
    cross = lax.rem(d + 2, 4)
    diag = 3 - d
    peers = (part, cross, diag)
    weights = {
        'qa': (wqa,), 'kva': (wka, wva), 'oa': (woa,), 'gua': (wga, wua), 'da': (wda,),
        'qb': (wqb,), 'kvb': (wkb, wvb), 'ob': (wob,), 'gub': (wgb, wub), 'db': (wdb,),
    }

    def cols(index):
        return pl.ds(pl.multiple_of(index * NC, NC), NC)

    def start_segment(name, first, m):
        slot = lax.rem(m, SP)
        i = m - first
        refs = weights[name]
        kind = name[:-1]
        if kind == 'q':
            for half in range(2):
                pltpu.make_async_copy(refs[0].at[:, cols(2 * i + half)], wbuf.at[slot, half], wsem.at[slot, half]).start()
        elif kind == 'kv':
            for half in range(2):
                pltpu.make_async_copy(refs[half], wbuf.at[slot, half], wsem.at[slot, half]).start()
        elif kind == 'gu':
            for half in range(2):
                pltpu.make_async_copy(refs[half].at[:, cols(i)], wbuf.at[slot, half], wsem.at[slot, half]).start()
        elif kind == 'd':
            for half in range(2):
                pltpu.make_async_copy(refs[0].at[:, cols(i + 8 * half)], wbuf.at[slot, half, pl.ds(0, FF)], wsem.at[slot, half]).start()
        else:
            for half in range(2):
                for sub in range(4):
                    pltpu.make_async_copy(refs[0].at[:, cols(4 * i + sub + 8 * half)],
                                          wbuf.at[slot, half, pl.ds(sub * WO_ROWS, WO_ROWS)], wsem.at[slot, half]).start()

    def issue(m, low, high):
        for name, first, count in SEGMENTS:
            if first >= high or first + count <= low:
                continue
            if first <= low and high <= first + count:
                start_segment(name, first, m)
            else:
                @pl.when(jnp.logical_and(m >= first, m < first + count))
                def _():
                    start_segment(name, first, m)

    def refill(m, low, high):
        if low + SP < TOTAL:
            issue(m + SP, low + SP, min(high + SP, TOTAL))

    def arrive(m, rows=D):
        slot = lax.rem(m, SP)
        for half in range(2):
            dst = wbuf.at[slot, half, pl.ds(0, rows)]
            pltpu.make_async_copy(dst, dst, wsem.at[slot, half]).wait()
        return slot

    def remote(src, dst, send, recv, to):
        return pltpu.make_async_remote_copy(src_ref=src, dst_ref=dst, send_sem=send, recv_sem=recv,
                                            device_id={'tp': to}, device_id_type=MESH)

    own_rows = pltpu.make_async_copy(hid.at[0], hx.at[d], lsem.at[0])
    own_rows.start()
    own_pos = pltpu.make_async_copy(pos, posb.at[d], lsem.at[1])
    own_pos.start()
    own_mask = pltpu.make_async_copy(tmask.at[0], maskb.at[d], lsem.at[2])
    own_mask.start()
    own_vis = pltpu.make_async_copy(vis.at[0], vg.at[d], lsem.at[3])
    own_vis.start()
    for m in range(SP):
        issue(m, m, m + 1)

    barrier = pltpu.get_barrier_semaphore()
    for peer in peers:
        pl.semaphore_signal(barrier, inc=1, device_id={'tp': peer}, device_id_type=MESH)
    pl.semaphore_wait(barrier, 3)

    own_rows.wait()
    own_pos.wait()
    own_mask.wait()
    first_sends = []
    for k, peer in enumerate(peers):
        first_sends.append(remote(hx.at[d], hx.at[d], hs.at[k], hr.at[k], peer))
        first_sends.append(remote(posb.at[d], posb.at[d], ps.at[k], pr.at[k], peer))
        first_sends.append(remote(maskb.at[d], maskb.at[d], ms.at[k], mr.at[k], peer))
    for copy in first_sends:
        copy.start()
    own_vis.wait()
    vis_part = remote(vg.at[d], vg.at[d], vs.at[0], vr.at[0], part)
    vis_part.start()

    def vis_half(block, n, index, to):
        rows = pl.ds(n * (VB // 2), VB // 2)
        return remote(vg.at[block, rows], vg.at[block, rows], vs.at[index], vr.at[index], to)

    vis_half(d, 0, 1, cross).start()

    for k, peer in enumerate(peers):
        remote(posb.at[peer], posb.at[peer], ps.at[k], pr.at[k], peer).wait_recv()
        remote(maskb.at[peer], maskb.at[peer], ms.at[k], mr.at[k], peer).wait_recv()

    lane = lax.broadcasted_iota(jnp.int32, (TB, HD), 1)
    sign = jnp.where(lane < HD // 2, -1.0, 1.0)
    eye = lax.broadcasted_iota(jnp.int32, (TB, TB), 0) == lax.broadcasted_iota(jnp.int32, (TB, TB), 1)
    freqs = freq[...]
    for block in range(4):
        row = posb[block].astype(F32)
        column = jnp.sum(jnp.where(eye, jnp.broadcast_to(row, (TB, TB)), 0.0), axis=1, keepdims=True)
        angles = column * freqs
        cosb[pl.ds(block * TB, TB), :] = jnp.cos(angles)
        sinb[pl.ds(block * TB, TB), :] = jnp.sin(angles) * sign

    for k, peer in enumerate(peers):
        remote(hx.at[peer], hx.at[peer], hs.at[k], hr.at[k], peer).wait_recv()

    for c in range(D // NC):
        h[c] = hx[:, :, c * NC:(c + 1) * NC].reshape(T, NC)

    def normalise(gain):
        total = jnp.zeros((T, NC), F32)
        for c in range(D // NC):
            v = h[c].astype(F32)
            total = total + v * v
        scale = lax.rsqrt(jnp.sum(total, axis=1, keepdims=True) * (1.0 / D) + NORM_EPS)
        for c in range(D // NC):
            g = gain[pl.ds(c * NC, NC)].astype(F32).reshape(1, NC)
            x[:, c * NC:(c + 1) * NC] = (h[c].astype(F32) * scale * g).astype(BF16)

    def head_norm(v, gain):
        scale = lax.rsqrt(jnp.mean(v * v, axis=1, keepdims=True) + NORM_EPS)
        return v * scale * gain[...].astype(F32).reshape(1, HD)

    def rope(v):
        return v * cosb[...] + pltpu.roll(v, HD // 2, 1) * sinb[...]

    def project(m, lhs):
        slot = arrive(m)
        return dot(lhs, wbuf[slot, 0]), dot(lhs, wbuf[slot, 1])

    def attend(keys, mask):
        for g in range(KV):
            q = qb[pl.ds(g * REP, REP)].reshape(REP * T, HD)
            scores = dot_t(q, kb[g, pl.ds(0, keys)]) * (HD ** -0.5)
            scores = jnp.where(mask, scores, MASK_VALUE)
            top = jnp.max(scores, axis=1, keepdims=True)
            e = jnp.exp(scores - top)
            p = (e / jnp.sum(e, axis=1, keepdims=True)).astype(BF16)
            o = dot(p, vb[g, pl.ds(0, keys)]).astype(BF16)
            for r in range(REP):
                head = g * REP + r
                ctx[:, head * HD:(head + 1) * HD] = o[r * T:(r + 1) * T]

    def reduce_all(parity, lag1, lag2, partials, update):
        def step(j, carry):
            @pl.when(j < 8)
            def _():
                low, high = partials(j)
                pb[0, j] = low.astype(BF16)
                pb[1, j] = high.astype(BF16)
                remote(pb.at[1 - core, j], rcv1.at[j], s1.at[j], r1.at[j], part).start()

            @pl.when(jnp.logical_and(j >= lag1, j < 8 + lag1))
            def _():
                i = j - lag1
                remote(pb.at[1 - core, i], rcv1.at[i], s1.at[i], r1.at[i], part).wait_recv()
                snd2[i] = (pb[core, i].astype(F32) + rcv1[i].astype(F32)).astype(BF16)
                remote(snd2.at[i], rcv2.at[parity, i], s2.at[parity, i], r2.at[parity, i], cross).start()

            @pl.when(j >= lag2)
            def _():
                i = j - lag2
                remote(snd2.at[i], rcv2.at[parity, i], s2.at[parity, i], r2.at[parity, i], cross).wait_recv()
                total = snd2[i].astype(F32) + rcv2[parity, i].astype(F32)
                mine = core * 8 + i
                h[mine] = (h[mine].astype(F32) + update(total)).astype(BF16)
                remote(h.at[mine], h.at[mine], s3.at[i], r3.at[i], part).start()
            return carry

        lax.fori_loop(0, 8 + lag2, step, 0)

        def finish(i, carry):
            theirs = (1 - core) * 8 + i
            mine = core * 8 + i
            remote(h.at[theirs], h.at[theirs], s3.at[i], r3.at[i], part).wait_recv()
            remote(h.at[mine], h.at[mine], s3.at[i], r3.at[i], part).wait_send()
            remote(pb.at[1 - core, i], rcv1.at[i], s1.at[i], r1.at[i], part).wait_send()
            remote(snd2.at[i], rcv2.at[parity, i], s2.at[parity, i], r2.at[parity, i], cross).wait_send()
            return carry

        return finish

    def wo_partials(base):
        def partials(j):
            m = base + j // 4
            sub = lax.rem(j, 4)
            slot = lax.rem(m, SP)

            @pl.when(sub == 0)
            def _():
                arrive(m)
            rows = pl.ds(pl.multiple_of(sub * WO_ROWS, WO_ROWS), WO_ROWS)
            low = dot(ctx[...], wbuf[slot, 0, rows])
            high = dot(ctx[...], wbuf[slot, 1, rows])

            @pl.when(sub == 3)
            def _():
                refill(m, base, base + 2)
            return low, high
        return partials

    def wd_partials(base):
        def partials(j):
            m = base + j
            slot = arrive(m, FF)
            rows = pl.ds(0, FF)
            low = dot(act[...], wbuf[slot, 0, rows])
            high = dot(act[...], wbuf[slot, 1, rows])
            refill(m, base, base + 8)
            return low, high
        return partials

    def mlp_up(base):
        def step(i, carry):
            m = base + i
            gate, up = project(m, x[...])
            act[:, cols(i)] = (gate * jax.nn.sigmoid(gate) * up).astype(BF16)
            refill(m, base, base + 14)
            return carry
        lax.fori_loop(0, 14, step, 0)

    normalise(ln1a)

    def q_step_a(i, carry):
        m = BASE['qa'] + i
        for half, q in enumerate(project(m, x[...])):
            for sub in range(2):
                qb[4 * i + 2 * half + sub] = rope(q[:, sub * HD:(sub + 1) * HD]).astype(BF16)
        refill(m, BASE['qa'], BASE['qa'] + 2)
        return carry

    lax.fori_loop(0, 2, q_step_a, 0)
    keys, vals = project(BASE['kva'], x[...])
    for g in range(KV):
        kb[g, pl.ds(0, T)] = rope(keys[:, g * HD:(g + 1) * HD]).astype(BF16)
        vb[g, pl.ds(0, T)] = vals[:, g * HD:(g + 1) * HD].astype(BF16)
    refill(BASE['kva'], BASE['kva'], BASE['kva'] + 1)
    query_at = lax.rem(lax.broadcasted_iota(jnp.int32, (REP * T, T), 0), T)
    attend(T, query_at >= lax.broadcasted_iota(jnp.int32, (REP * T, T), 1))
    lax.fori_loop(0, 8, reduce_all(0, 3, 7, wo_partials(BASE['oa']), lambda total: total), 0)
    vis_half(d, 1, 2, cross).start()
    normalise(ln2a)
    mlp_up(BASE['gua'])
    for n in range(2):
        vis_half(cross, n, 1 + n, cross).wait_recv()
        vis_half(cross, n, 3 + n, part).start()
    end_a = reduce_all(1, 1, 4, wd_partials(BASE['da']), lambda total: total)

    remote(vg.at[part], vg.at[part], vs.at[0], vr.at[0], part).wait_recv()
    for n in range(2):
        vis_half(diag, n, 3 + n, part).wait_recv()
    slot_kv = arrive(BASE['kvb'])

    def kv_step(block, carry):
        rows = pl.ds(pl.multiple_of(block * VB, VB), VB)
        keys = dot(vg[block], wbuf[slot_kv, 0])
        vals = dot(vg[block], wbuf[slot_kv, 1])
        for g in range(KV):
            kb[g, rows] = head_norm(keys[:, g * HD:(g + 1) * HD], kn).astype(BF16)
            vb[g, rows] = vals[:, g * HD:(g + 1) * HD].astype(BF16)
        return carry

    lax.fori_loop(0, 4, kv_step, 0)
    refill(BASE['kvb'], BASE['kvb'], BASE['kvb'] + 1)
    lax.fori_loop(0, 8, end_a, 0)
    normalise(ln1b)

    def q_step_b(i, carry):
        m = BASE['qb'] + i
        for half, q in enumerate(project(m, x[...])):
            for sub in range(2):
                qb[4 * i + 2 * half + sub] = head_norm(q[:, sub * HD:(sub + 1) * HD], qn).astype(BF16)
        refill(m, BASE['qb'], BASE['qb'] + 2)
        return carry

    lax.fori_loop(0, 2, q_step_b, 0)
    seen = (maskb[...].reshape(T, 4) > 0).astype(F32)
    tile_at = lax.broadcasted_iota(jnp.int32, (T, V), 1) // (V // 4)
    visible = jnp.zeros((T, V), F32)
    for tile in range(4):
        visible = jnp.where(tile_at == tile, jnp.broadcast_to(seen[:, tile:tile + 1], (T, V)), visible)
    attend(V, jnp.concatenate([visible] * REP, axis=0) > 0.0)
    keep = jnp.max(seen, axis=1, keepdims=True)
    gate0 = jnp.tanh(jnp.full((T, 1), xg[0], F32)) * keep
    lax.fori_loop(0, 8, reduce_all(2, 3, 7, wo_partials(BASE['ob']), lambda total: gate0 * total), 0)
    normalise(ln2b)
    mlp_up(BASE['gub'])

    own_seen = (maskb[d] > 0).astype(F32)
    gate1 = jnp.tanh(jnp.full((TB, 1), xg[1], F32)) * jnp.max(own_seen, axis=1, keepdims=True)
    down = wd_partials(BASE['db'])
    lag = 3

    def last_step(j, carry):
        @pl.when(j < 8)
        def _():
            for half, value in enumerate(down(j)):
                pf[j, :, half] = value.astype(BF16).reshape(4, TB, NC)
            for k, peer in enumerate(peers):
                remote(pf.at[j, peer], rcvf.at[j, k], fs.at[j, k], fr.at[j, k], peer).start()

        @pl.when(j >= lag)
        def _():
            i = j - lag
            for k, peer in enumerate(peers):
                remote(pf.at[i, peer], rcvf.at[i, k], fs.at[i, k], fr.at[i, k], peer).wait_recv()
            for half in range(2):
                total = pf[i, d, half].astype(F32)
                for k in range(3):
                    total = total + rcvf[i, k, half].astype(F32)
                chunk = i + 8 * half
                rows = pl.ds(pl.multiple_of(d * TB, TB), TB)
                out[0, :, cols(chunk)] = (h[chunk, rows].astype(F32) + gate1 * total).astype(BF16)
        return carry

    lax.fori_loop(0, 8 + lag, last_step, 0)

    for copy in first_sends:
        copy.wait_send()
    vis_part.wait_send()
    for n in range(2):
        vis_half(d, n, 1 + n, cross).wait_send()
        vis_half(cross, n, 3 + n, part).wait_send()

    def drain(j, carry):
        for k, peer in enumerate(peers):
            remote(pf.at[j, peer], rcvf.at[j, k], fs.at[j, k], fr.at[j, k], peer).wait_send()
        return carry

    lax.fori_loop(0, 8, drain, 0)


def solution(mesh):
    act_spec = P('dp', 'tp', None)
    col_spec = P(None, 'tp')
    row_spec = P('tp', None)
    layer_a = (P(), col_spec, col_spec, col_spec, row_spec, P(), col_spec, col_spec, row_spec)
    layer_b = (P(), col_spec, P(), col_spec, col_spec, P(), row_spec, P(), col_spec, col_spec, row_spec, P())
    in_specs = (act_spec, act_spec, P('dp', 'tp'), act_spec) + layer_a + layer_b
    table = rope_table(HD)

    hbm = pl.BlockSpec(memory_space=pl.ANY)
    vmem = pl.BlockSpec(memory_space=pltpu.VMEM)
    smem = pl.BlockSpec(memory_space=pltpu.SMEM)
    dma = pltpu.SemaphoreType.DMA
    scratch = [
        pltpu.VMEM((SP, 2, D, NC), BF16), dma((SP, 2)),
        pltpu.VMEM((4, TB, D), BF16),
        pltpu.VMEM((4, 1, TB), jnp.int32),
        pltpu.VMEM((4, TB, 4), jnp.int32),
        pltpu.VMEM((T, HD), F32), pltpu.VMEM((T, HD), F32),
        pltpu.VMEM((D // NC, T, NC), BF16),
        pltpu.VMEM((T, D), BF16),
        pltpu.VMEM((T, FF), BF16),
        pltpu.VMEM((T, WO_ROWS), BF16),
        pltpu.VMEM((KV * REP, T, HD), BF16),
        pltpu.VMEM((KV, V, HD), BF16), pltpu.VMEM((KV, V, HD), BF16),
        pltpu.VMEM((4, VB, D), BF16),
        pltpu.VMEM((2, 8, T, NC), BF16),
        pltpu.VMEM((8, T, NC), BF16),
        pltpu.VMEM((8, T, NC), BF16),
        pltpu.VMEM((3, 8, T, NC), BF16),
        pltpu.VMEM((8, 4, 2, TB, NC), BF16),
        pltpu.VMEM((8, 3, 2, TB, NC), BF16),
        dma((4,)),
        dma((3,)), dma((3,)), dma((3,)), dma((3,)), dma((3,)), dma((3,)),
        dma((5,)), dma((5,)),
        dma((8,)), dma((8,)), dma((3, 8)), dma((3, 8)), dma((8,)), dma((8,)),
        dma((8, 3)), dma((8, 3)),
    ]

    def body(hidden, vision, positions, tile_mask, *params):
        freqs = jnp.asarray(np.concatenate([table, table])[None])
        specs = [hbm, hbm, hbm, hbm, vmem]
        for k, p in enumerate(params):
            specs.append(vmem if p.ndim == 1 else hbm)
        specs[-1] = smem
        return pl.pallas_call(
            kernel,
            out_shape=jax.ShapeDtypeStruct(hidden.shape, BF16),
            in_specs=specs,
            out_specs=vmem,
            scratch_shapes=scratch,
            compiler_params=pltpu.CompilerParams(
                collective_id=0, has_side_effects=True, vmem_limit_bytes=67043328),
            cost_estimate=pl.CostEstimate(flops=2 * 64 * 109051904, bytes_accessed=218103808, transcendentals=0),
            name='layers',
        )(hidden, vision, positions, tile_mask, freqs, *params)

    return jax.shard_map(body, mesh=mesh, in_specs=in_specs, out_specs=act_spec, check_vma=False)
```

```python
import math
import jax
import jax.numpy as jnp
import numpy as np
from jax import lax
from jax.experimental import pallas as pl
from jax.experimental.pallas import tpu as pltpu
from jax.sharding import PartitionSpec as P

ROPE_THETA = 500000.0
ROPE_FACTOR = 8.0
LOW_FACTOR = 1.0
HIGH_FACTOR = 4.0
ORIG_CONTEXT = 8192.0
NORM_EPS = 1e-5
MASK_VALUE = -1e30
MESH = pl.DeviceIdType.MESH
BF16 = jnp.bfloat16
F32 = jnp.float32

T = 64
TB = 16
D = 4096
V = 256
VB = 64
HD = 128
KV = 2
REP = 4
FF = 3584
NC = 256
SP = 13
WO_ROWS = KV * REP * HD

SEGMENTS = []
_at = 0
for _name, _count in (('qa', 2), ('kva', 1), ('oa', 2), ('gua', 14), ('da', 8),
                      ('kvb', 1), ('qb', 2), ('ob', 2), ('gub', 14), ('db', 8)):
    SEGMENTS.append((_name, _at, _count))
    _at += _count
TOTAL = _at
BASE = {name: first for name, first, _ in SEGMENTS}


def rope_table(head_dim):
    low_wave = ORIG_CONTEXT / LOW_FACTOR
    high_wave = ORIG_CONTEXT / HIGH_FACTOR
    freq_list = []
    for freq_idx in range(head_dim // 2):
        base_freq = 1.0 / (ROPE_THETA ** (2.0 * freq_idx / head_dim))
        wave_len = 2.0 * math.pi / base_freq
        if wave_len > low_wave:
            freq_list.append(base_freq / ROPE_FACTOR)
        elif wave_len < high_wave:
            freq_list.append(base_freq)
        else:
            smooth = (ORIG_CONTEXT / wave_len - LOW_FACTOR) / (HIGH_FACTOR - LOW_FACTOR)
            freq_list.append((1.0 - smooth) * base_freq / ROPE_FACTOR + smooth * base_freq)
    return np.array(freq_list, dtype=np.float32)


def dot(a, b):
    return jnp.dot(a, b, preferred_element_type=F32)


def dot_t(a, b):
    return lax.dot_general(a, b, (((1,), (1,)), ((), ())), preferred_element_type=F32)


def kernel(hid, vis, pos, tmask, freq,
           ln1a, wqa, wka, wva, woa, ln2a, wga, wua, wda,
           ln1b, wqb, qn, wkb, wvb, kn, wob, ln2b, wgb, wub, wdb, xg,
           out,
           wbuf, wsem, hx, posb, maskb, cosb, sinb, visb, keepb, h, x, act, ctx, qb, kb, vb, vg,
           pb, rcv1, snd2, rcv2, pf, rcvf,
           lsem, hs, hr, ps, pr, ms, mr, vs, vr, s1, r1, s2, r2, s3, r3, fs, fr):
    d = lax.axis_index('tp')
    core = lax.rem(d, 2)
    part = d + 1 - 2 * core
    cross = lax.rem(d + 2, 4)
    diag = 3 - d
    peers = (part, cross, diag)
    weights = {
        'qa': (wqa,), 'kva': (wka, wva), 'oa': (woa,), 'gua': (wga, wua), 'da': (wda,),
        'qb': (wqb,), 'kvb': (wkb, wvb), 'ob': (wob,), 'gub': (wgb, wub), 'db': (wdb,),
    }

    def cols(index):
        return pl.ds(pl.multiple_of(index * NC, NC), NC)

    def start_segment(name, first, m):
        slot = lax.rem(m, SP)
        i = m - first
        refs = weights[name]
        kind = name[:-1]
        if kind == 'q':
            for half in range(2):
                pltpu.make_async_copy(refs[0].at[:, cols(2 * i + half)], wbuf.at[slot, half], wsem.at[slot, half]).start()
        elif kind == 'kv':
            for half in range(2):
                pltpu.make_async_copy(refs[half], wbuf.at[slot, half], wsem.at[slot, half]).start()
        elif kind == 'gu':
            for half in range(2):
                pltpu.make_async_copy(refs[half].at[:, cols(i)], wbuf.at[slot, half], wsem.at[slot, half]).start()
        elif kind == 'd':
            for half in range(2):
                pltpu.make_async_copy(refs[0].at[:, cols(i + 8 * half)], wbuf.at[slot, half, pl.ds(0, FF)], wsem.at[slot, half]).start()
        else:
            for half in range(2):
                for sub in range(4):
                    pltpu.make_async_copy(refs[0].at[:, cols(4 * i + sub + 8 * half)],
                                          wbuf.at[slot, half, pl.ds(sub * WO_ROWS, WO_ROWS)], wsem.at[slot, half]).start()

    def issue(m, low, high):
        for name, first, count in SEGMENTS:
            if first >= high or first + count <= low:
                continue
            if first <= low and high <= first + count:
                start_segment(name, first, m)
            else:
                @pl.when(jnp.logical_and(m >= first, m < first + count))
                def _():
                    start_segment(name, first, m)

    def refill(m, low, high):
        if low + SP < TOTAL:
            issue(m + SP, low + SP, high + SP)

    def arrive(m, rows=D):
        slot = lax.rem(m, SP)
        for half in range(2):
            dst = wbuf.at[slot, half, pl.ds(0, rows)]
            pltpu.make_async_copy(dst, dst, wsem.at[slot, half]).wait()
        return slot

    def remote(src, dst, send, recv, to):
        return pltpu.make_async_remote_copy(src_ref=src, dst_ref=dst, send_sem=send, recv_sem=recv,
                                            device_id={'tp': to}, device_id_type=MESH)

    own_rows = pltpu.make_async_copy(hid.at[0], hx.at[d], lsem.at[0])
    own_rows.start()
    own_pos = pltpu.make_async_copy(pos, posb.at[d], lsem.at[1])
    own_pos.start()
    own_mask = pltpu.make_async_copy(tmask.at[0], maskb.at[d], lsem.at[2])
    own_mask.start()
    barrier = pltpu.get_barrier_semaphore()
    for peer in peers:
        pl.semaphore_signal(barrier, inc=1, device_id={'tp': peer}, device_id_type=MESH)
    for m in range(4):
        issue(m, m, m + 1)
    own_vis = pltpu.make_async_copy(vis.at[0], vg.at[d], lsem.at[3])
    own_vis.start()
    for m in range(4, SP):
        issue(m, m, m + 1)
    own_rows.wait()
    own_pos.wait()
    own_mask.wait()
    pl.semaphore_wait(barrier, 3)

    def hid_half(block, n, index, to):
        rows = pl.ds(n * (TB // 2), TB // 2)
        return remote(hx.at[block, rows], hx.at[block, rows], hs.at[index], hr.at[index], to)

    def vis_half(block, n, index, to):
        rows = pl.ds(n * (VB // 2), VB // 2)
        return remote(vg.at[block, rows], vg.at[block, rows], vs.at[index], vr.at[index], to)

    first_sends = [hid_half(d, 0, 1, cross), hid_half(d, 1, 2, cross), remote(hx.at[d], hx.at[d], hs.at[0], hr.at[0], part)]
    for k, peer in enumerate(peers):
        first_sends.append(remote(posb.at[d], posb.at[d], ps.at[k], pr.at[k], peer))
        first_sends.append(remote(maskb.at[d], maskb.at[d], ms.at[k], mr.at[k], peer))
    for copy in first_sends:
        copy.start()
    own_vis.wait()
    vis_part = remote(vg.at[d], vg.at[d], vs.at[0], vr.at[0], part)
    vis_part.start()
    vis_half(d, 0, 1, cross).start()

    for k, peer in enumerate(peers):
        remote(posb.at[peer], posb.at[peer], ps.at[k], pr.at[k], peer).wait_recv()
        remote(maskb.at[peer], maskb.at[peer], ms.at[k], mr.at[k], peer).wait_recv()

    sign = jnp.where(lax.broadcasted_iota(jnp.int32, (TB, HD), 1) < HD // 2, -1.0, 1.0)
    eye = lax.broadcasted_iota(jnp.int32, (TB, TB), 0) == lax.broadcasted_iota(jnp.int32, (TB, TB), 1)
    freqs = freq[...]

    def as_column(row):
        return jnp.sum(jnp.where(eye, jnp.broadcast_to(row, (TB, TB)), 0.0), axis=1, keepdims=True)

    for block in range(4):
        rows = pl.ds(block * TB, TB)
        angles = as_column(posb[block].astype(F32)) * freqs
        cosb[rows, :] = jnp.cos(angles)
        sinb[rows, :] = jnp.sin(angles) * sign
        seen = (maskb[block] > 0).astype(F32)
        for tile in range(4):
            visb[rows, tile * (V // 4):(tile + 1) * (V // 4)] = jnp.broadcast_to(as_column(seen[tile:tile + 1]), (TB, V // 4))
        keepb[rows, :] = jnp.broadcast_to(as_column(jnp.max(seen, axis=0, keepdims=True)), (TB, HD))

    for n in range(2):
        hid_half(cross, n, 1 + n, cross).wait_recv()
        hid_half(cross, n, 3 + n, part).start()
    remote(hx.at[part], hx.at[part], hs.at[0], hr.at[0], part).wait_recv()
    for n in range(2):
        hid_half(diag, n, 3 + n, part).wait_recv()

    for c in range(D // NC):
        h[c] = hx[:, :, c * NC:(c + 1) * NC].reshape(T, NC)

    def normalise(gain):
        total = jnp.zeros((T, NC), F32)
        for c in range(D // NC):
            v = h[c].astype(F32)
            total = total + v * v
        scale = lax.rsqrt(jnp.sum(total, axis=1, keepdims=True) * (1.0 / D) + NORM_EPS)
        for c in range(D // NC):
            g = gain[pl.ds(c * NC, NC)].astype(F32).reshape(1, NC)
            x[:, c * NC:(c + 1) * NC] = (h[c].astype(F32) * scale * g).astype(BF16)

    def head_norm(v, gain):
        scale = lax.rsqrt(jnp.mean(v * v, axis=1, keepdims=True) + NORM_EPS)
        return v * scale * gain[...].astype(F32).reshape(1, HD)

    def rope(v):
        return v * cosb[...] + pltpu.roll(v, HD // 2, 1) * sinb[...]

    def attend(keys, mask):
        for g in range(KV):
            q = qb[pl.ds(g * REP, REP)].reshape(REP * T, HD)
            scores = dot_t(q, kb[g, pl.ds(0, keys)]) * (HD ** -0.5)
            scores = jnp.where(mask, scores, MASK_VALUE)
            top = jnp.max(scores, axis=1, keepdims=True)
            e = jnp.exp(scores - top)
            p = (e / jnp.sum(e, axis=1, keepdims=True)).astype(BF16)
            o = dot(p, vb[g, pl.ds(0, keys)]).astype(BF16)
            for r in range(REP):
                head = g * REP + r
                ctx[:, head * HD:(head + 1) * HD] = o[r * T:(r + 1) * T]

    def spread(parity, partials, update, between=None):
        def hop1(i):
            return remote(pb.at[1 - core, i], rcv1.at[i], s1.at[i], r1.at[i], part)

        def hop2(i):
            return remote(snd2.at[i], rcv2.at[parity, i], s2.at[parity, i], r2.at[parity, i], cross)

        def hop3(half, i):
            return remote(h.at[half * 8 + i], h.at[half * 8 + i], s3.at[i], r3.at[i], part)

        def fold(i):
            hop1(i).wait_recv()
            snd2[i] = (pb[core, i].astype(F32) + rcv1[i].astype(F32)).astype(BF16)
            hop2(i).start()

        def step(j, carry):
            for n, (low, high) in enumerate(partials(j)):
                i = 2 * j + n
                pb[0, i] = low.astype(BF16)
                pb[1, i] = high.astype(BF16)
                hop1(i).start()

            @pl.when(j >= 1)
            def _():
                fold(2 * j - 2)
                fold(2 * j - 1)
            return carry

        lax.fori_loop(0, 4, step, 0)
        fold(6)
        fold(7)
        if between is not None:
            between()

        def final(i, carry):
            hop2(i).wait_recv()
            total = snd2[i].astype(F32) + rcv2[parity, i].astype(F32)
            mine = core * 8 + i
            h[mine] = (h[mine].astype(F32) + update(total)).astype(BF16)
            hop3(core, i).start()
            return carry

        lax.fori_loop(0, 8, final, 0)

        def finish(i, carry):
            hop3(1 - core, i).wait_recv()
            hop3(core, i).wait_send()
            hop1(i).wait_send()
            hop2(i).wait_send()
            return carry

        lax.fori_loop(0, 8, finish, 0)

    def wo_partials(base):
        def partials(j):
            m = base + j // 2
            slot = lax.rem(m, SP)

            @pl.when(lax.rem(j, 2) == 0)
            def _():
                arrive(m)
            out = []
            for n in range(2):
                rows = pl.ds(pl.multiple_of((lax.rem(j, 2) * 2 + n) * WO_ROWS, WO_ROWS), WO_ROWS)
                out.append((dot(ctx[...], wbuf[slot, 0, rows]), dot(ctx[...], wbuf[slot, 1, rows])))

            @pl.when(lax.rem(j, 2) == 1)
            def _():
                refill(m, base, base + 2)
            return out
        return partials

    def wd_partials(base):
        def partials(j):
            slots = [arrive(base + 2 * j + n, FF) for n in range(2)]
            out = []
            for slot in slots:
                rows = pl.ds(0, FF)
                out.append((dot(act[...], wbuf[slot, 0, rows]), dot(act[...], wbuf[slot, 1, rows])))
            for n in range(2):
                refill(base + 2 * j + n, base, base + 8)
            return out
        return partials

    def mlp_up(base):
        def step(i, carry):
            slots = [arrive(base + 2 * i + n) for n in range(2)]
            for n, slot in enumerate(slots):
                gate = dot(x[...], wbuf[slot, 0])
                up = dot(x[...], wbuf[slot, 1])
                act[:, cols(2 * i + n)] = (gate * jax.nn.sigmoid(gate) * up).astype(BF16)
            for n in range(2):
                refill(base + 2 * i + n, base, base + 14)
            return carry
        lax.fori_loop(0, 7, step, 0)

    def queries(base, finish):
        slots = [arrive(base + i) for i in range(2)]
        for i, slot in enumerate(slots):
            for half in range(2):
                q = dot(x[...], wbuf[slot, half])
                for sub in range(2):
                    qb[4 * i + 2 * half + sub] = finish(q[:, sub * HD:(sub + 1) * HD]).astype(BF16)

    normalise(ln1a)
    slot_kv = arrive(BASE['kva'])
    queries(BASE['qa'], rope)
    keys, vals = dot(x[...], wbuf[slot_kv, 0]), dot(x[...], wbuf[slot_kv, 1])
    for g in range(KV):
        kb[g, pl.ds(0, T)] = rope(keys[:, g * HD:(g + 1) * HD]).astype(BF16)
        vb[g, pl.ds(0, T)] = vals[:, g * HD:(g + 1) * HD].astype(BF16)
    for m in range(3):
        refill(m, m, m + 1)
    query_at = lax.rem(lax.broadcasted_iota(jnp.int32, (REP * T, T), 0), T)
    attend(T, query_at >= lax.broadcasted_iota(jnp.int32, (REP * T, T), 1))
    spread(0, wo_partials(BASE['oa']), lambda total: total)
    vis_half(d, 1, 2, cross).start()
    normalise(ln2a)
    mlp_up(BASE['gua'])
    for n in range(2):
        vis_half(cross, n, 1 + n, cross).wait_recv()
        vis_half(cross, n, 3 + n, part).start()

    def vision_heads():
        remote(vg.at[part], vg.at[part], vs.at[0], vr.at[0], part).wait_recv()
        for n in range(2):
            vis_half(diag, n, 3 + n, part).wait_recv()
        slot = arrive(BASE['kvb'])

        def kv_step(n, carry):
            rows = pl.ds(pl.multiple_of(n * 2 * VB, 2 * VB), 2 * VB)
            lhs = vg[pl.ds(2 * n, 2)].reshape(2 * VB, D)
            keys = dot(lhs, wbuf[slot, 0])
            vals = dot(lhs, wbuf[slot, 1])
            for g in range(KV):
                kb[g, rows] = head_norm(keys[:, g * HD:(g + 1) * HD], kn).astype(BF16)
                vb[g, rows] = vals[:, g * HD:(g + 1) * HD].astype(BF16)
            return carry

        lax.fori_loop(0, 2, kv_step, 0)
        refill(BASE['kvb'], BASE['kvb'], BASE['kvb'] + 1)

    spread(1, wd_partials(BASE['da']), lambda total: total, vision_heads)

    normalise(ln1b)
    queries(BASE['qb'], lambda q: head_norm(q, qn))
    for i in range(2):
        refill(BASE['qb'] + i, BASE['qb'] + i, BASE['qb'] + i + 1)
    attend(V, jnp.concatenate([visb[...]] * REP, axis=0) > 0.0)
    gate0 = jnp.tanh(jnp.full((T, 1), xg[0], F32)) * keepb[:, 0:1]
    spread(2, wo_partials(BASE['ob']), lambda total: gate0 * total)
    normalise(ln2b)
    mlp_up(BASE['gub'])

    own = pl.ds(pl.multiple_of(d * TB, TB), TB)
    gate1 = jnp.tanh(jnp.full((TB, 1), xg[1], F32)) * keepb[own, 0:1]
    down = wd_partials(BASE['db'])

    def last_step(j, carry):
        for n, values in enumerate(down(j)):
            i = 2 * j + n
            for half, value in enumerate(values):
                pf[i, :, half] = value.astype(BF16).reshape(4, TB, NC)
            for k, peer in enumerate(peers):
                remote(pf.at[i, peer], rcvf.at[i, k], fs.at[i, k], fr.at[i, k], peer).start()
        return carry

    lax.fori_loop(0, 4, last_step, 0)

    def last_sum(i, carry):
        for k, peer in enumerate(peers):
            remote(pf.at[i, peer], rcvf.at[i, k], fs.at[i, k], fr.at[i, k], peer).wait_recv()
        for half in range(2):
            total = pf[i, d, half].astype(F32)
            for k in range(3):
                total = total + rcvf[i, k, half].astype(F32)
            chunk = i + 8 * half
            out[0, :, cols(chunk)] = (h[chunk, own].astype(F32) + gate1 * total).astype(BF16)
        return carry

    lax.fori_loop(0, 8, last_sum, 0)

    for copy in first_sends:
        copy.wait_send()
    vis_part.wait_send()
    for n in range(2):
        hid_half(cross, n, 3 + n, part).wait_send()
        vis_half(d, n, 1 + n, cross).wait_send()
        vis_half(cross, n, 3 + n, part).wait_send()

    def drain(j, carry):
        for k, peer in enumerate(peers):
            remote(pf.at[j, peer], rcvf.at[j, k], fs.at[j, k], fr.at[j, k], peer).wait_send()
        return carry

    lax.fori_loop(0, 8, drain, 0)


def solution(mesh):
    act_spec = P('dp', 'tp', None)
    col_spec = P(None, 'tp')
    row_spec = P('tp', None)
    layer_a = (P(), col_spec, col_spec, col_spec, row_spec, P(), col_spec, col_spec, row_spec)
    layer_b = (P(), col_spec, P(), col_spec, col_spec, P(), row_spec, P(), col_spec, col_spec, row_spec, P())
    in_specs = (act_spec, act_spec, P('dp', 'tp'), act_spec) + layer_a + layer_b
    table = rope_table(HD)

    hbm = pl.BlockSpec(memory_space=pl.ANY)
    vmem = pl.BlockSpec(memory_space=pltpu.VMEM)
    smem = pl.BlockSpec(memory_space=pltpu.SMEM)
    dma = pltpu.SemaphoreType.DMA
    scratch = [
        pltpu.VMEM((SP, 2, D, NC), BF16), dma((SP, 2)),
        pltpu.VMEM((4, TB, D), BF16),
        pltpu.VMEM((4, 1, TB), jnp.int32),
        pltpu.VMEM((4, 4, TB), jnp.int32),
        pltpu.VMEM((T, HD), F32), pltpu.VMEM((T, HD), F32),
        pltpu.VMEM((T, V), F32), pltpu.VMEM((T, HD), F32),
        pltpu.VMEM((D // NC, T, NC), BF16),
        pltpu.VMEM((T, D), BF16),
        pltpu.VMEM((T, FF), BF16),
        pltpu.VMEM((T, WO_ROWS), BF16),
        pltpu.VMEM((KV * REP, T, HD), BF16),
        pltpu.VMEM((KV, V, HD), BF16), pltpu.VMEM((KV, V, HD), BF16),
        pltpu.VMEM((4, VB, D), BF16),
        pltpu.VMEM((2, 8, T, NC), BF16),
        pltpu.VMEM((8, T, NC), BF16),
        pltpu.VMEM((8, T, NC), BF16),
        pltpu.VMEM((3, 8, T, NC), BF16),
        pltpu.VMEM((8, 4, 2, TB, NC), BF16),
        pltpu.VMEM((8, 3, 2, TB, NC), BF16),
        dma((4,)),
        dma((5,)), dma((5,)), dma((3,)), dma((3,)), dma((3,)), dma((3,)),
        dma((5,)), dma((5,)),
        dma((8,)), dma((8,)), dma((3, 8)), dma((3, 8)), dma((8,)), dma((8,)),
        dma((8, 3)), dma((8, 3)),
    ]

    def body(hidden, vision, positions, tile_mask, *params):
        freqs = jnp.asarray(np.concatenate([table, table])[None])
        specs = [hbm, hbm, hbm, hbm, vmem]
        for k, p in enumerate(params):
            specs.append(vmem if p.ndim == 1 else hbm)
        specs[-1] = smem
        return pl.pallas_call(
            kernel,
            out_shape=jax.ShapeDtypeStruct(hidden.shape, BF16),
            in_specs=specs,
            out_specs=vmem,
            scratch_shapes=scratch,
            compiler_params=pltpu.CompilerParams(
                collective_id=0, has_side_effects=True, vmem_limit_bytes=67043328),
            cost_estimate=pl.CostEstimate(flops=2 * 64 * 109051904, bytes_accessed=218103808, transcendentals=0),
            name='layers',
        )(hidden, vision, positions, jnp.swapaxes(tile_mask, 1, 2), freqs, *params)

    return jax.shard_map(body, mesh=mesh, in_specs=in_specs, out_specs=act_spec, check_vma=False)
```

```python
import math
import jax
import jax.numpy as jnp
import numpy as np
from jax import lax
from jax.experimental import pallas as pl
from jax.experimental.pallas import tpu as pltpu
from jax.sharding import PartitionSpec as P

ROPE_THETA = 500000.0
ROPE_FACTOR = 8.0
LOW_FACTOR = 1.0
HIGH_FACTOR = 4.0
ORIG_CONTEXT = 8192.0
NORM_EPS = 1e-5
MASK_VALUE = -1e30
MESH = pl.DeviceIdType.MESH
BF16 = jnp.bfloat16
F32 = jnp.float32

T = 64
TB = 16
D = 4096
V = 256
VB = 64
HD = 128
KV = 2
REP = 4
FF = 3584
NC = 256
SP = 13
WO_ROWS = KV * REP * HD

SEGMENTS = []
_at = 0
for _name, _count in (('qa', 2), ('kva', 1), ('oa', 2), ('gua', 14), ('da', 8),
                      ('kvb', 1), ('qb', 2), ('ob', 2), ('gub', 14), ('db', 8)):
    SEGMENTS.append((_name, _at, _count))
    _at += _count
TOTAL = _at
BASE = {name: first for name, first, _ in SEGMENTS}


def rope_table(head_dim):
    low_wave = ORIG_CONTEXT / LOW_FACTOR
    high_wave = ORIG_CONTEXT / HIGH_FACTOR
    freq_list = []
    for freq_idx in range(head_dim // 2):
        base_freq = 1.0 / (ROPE_THETA ** (2.0 * freq_idx / head_dim))
        wave_len = 2.0 * math.pi / base_freq
        if wave_len > low_wave:
            freq_list.append(base_freq / ROPE_FACTOR)
        elif wave_len < high_wave:
            freq_list.append(base_freq)
        else:
            smooth = (ORIG_CONTEXT / wave_len - LOW_FACTOR) / (HIGH_FACTOR - LOW_FACTOR)
            freq_list.append((1.0 - smooth) * base_freq / ROPE_FACTOR + smooth * base_freq)
    return np.array(freq_list, dtype=np.float32)


def dot(a, b):
    return jnp.dot(a, b, preferred_element_type=F32)


def dot_t(a, b):
    return lax.dot_general(a, b, (((1,), (1,)), ((), ())), preferred_element_type=F32)


def kernel(hid, vis, pos, tmask, freq,
           ln1a, wqa, wka, wva, woa, ln2a, wga, wua, wda,
           ln1b, wqb, qn, wkb, wvb, kn, wob, ln2b, wgb, wub, wdb, xg,
           out,
           wbuf, wsem, hx, posb, maskb, cosb, sinb, visb, keepb, h, x, act, ctx, qb, kb, vb, vg,
           pb, rcv1, snd2, rcv2, pf, rcvf, obuf, osem,
           lsem, hs, hr, ps, pr, ms, mr, vs, vr, s1, r1, s2, r2, s3, r3, fs, fr):
    d = lax.axis_index('tp')
    core = lax.rem(d, 2)
    part = d + 1 - 2 * core
    cross = lax.rem(d + 2, 4)
    diag = 3 - d
    peers = (part, cross, diag)
    weights = {
        'qa': (wqa,), 'kva': (wka, wva), 'oa': (woa,), 'gua': (wga, wua), 'da': (wda,),
        'qb': (wqb,), 'kvb': (wkb, wvb), 'ob': (wob,), 'gub': (wgb, wub), 'db': (wdb,),
    }

    def cols(index):
        return pl.ds(pl.multiple_of(index * NC, NC), NC)

    def start_segment(name, first, m):
        slot = lax.rem(m, SP)
        i = m - first
        refs = weights[name]
        kind = name[:-1]
        if kind == 'q':
            for half in range(2):
                pltpu.make_async_copy(refs[0].at[:, cols(2 * i + half)], wbuf.at[slot, half], wsem.at[slot, half]).start()
        elif kind == 'kv':
            for half in range(2):
                pltpu.make_async_copy(refs[half], wbuf.at[slot, half], wsem.at[slot, half]).start()
        elif kind == 'gu':
            for half in range(2):
                pltpu.make_async_copy(refs[half].at[:, cols(i)], wbuf.at[slot, half], wsem.at[slot, half]).start()
        elif kind == 'd':
            for half in range(2):
                pltpu.make_async_copy(refs[0].at[:, cols(i + 8 * half)], wbuf.at[slot, half, pl.ds(0, FF)], wsem.at[slot, half]).start()
        else:
            for half in range(2):
                for sub in range(4):
                    pltpu.make_async_copy(refs[0].at[:, cols(4 * i + sub + 8 * half)],
                                          wbuf.at[slot, half, pl.ds(sub * WO_ROWS, WO_ROWS)], wsem.at[slot, half]).start()

    def issue(m, low, high):
        for name, first, count in SEGMENTS:
            if first >= high or first + count <= low:
                continue
            if first <= low and high <= first + count:
                start_segment(name, first, m)
            else:
                @pl.when(jnp.logical_and(m >= first, m < first + count))
                def _():
                    start_segment(name, first, m)

    def refill(m, low, high):
        if low + SP < TOTAL:
            issue(m + SP, low + SP, high + SP)

    def arrive(m, rows=D):
        slot = lax.rem(m, SP)
        for half in range(2):
            dst = wbuf.at[slot, half, pl.ds(0, rows)]
            pltpu.make_async_copy(dst, dst, wsem.at[slot, half]).wait()
        return slot

    def remote(src, dst, send, recv, to):
        return pltpu.make_async_remote_copy(src_ref=src, dst_ref=dst, send_sem=send, recv_sem=recv,
                                            device_id={'tp': to}, device_id_type=MESH)

    own_rows = pltpu.make_async_copy(hid.at[0], hx.at[d], lsem.at[0])
    own_rows.start()
    own_pos = pltpu.make_async_copy(pos, posb.at[d], lsem.at[1])
    own_pos.start()
    own_mask = pltpu.make_async_copy(tmask.at[0], maskb.at[d], lsem.at[2])
    own_mask.start()
    own_vis = pltpu.make_async_copy(vis.at[0], vg.at[d], lsem.at[3])
    own_vis.start()
    barrier = pltpu.get_barrier_semaphore()
    for peer in peers:
        pl.semaphore_signal(barrier, inc=1, device_id={'tp': peer}, device_id_type=MESH)
    for m in range(4):
        issue(m, m, m + 1)
    own_rows.wait()
    own_pos.wait()
    own_mask.wait()
    pl.semaphore_wait(barrier, 3)

    def hid_half(block, n, index, to):
        rows = pl.ds(n * (TB // 2), TB // 2)
        return remote(hx.at[block, rows], hx.at[block, rows], hs.at[index], hr.at[index], to)

    def vis_half(block, n, index, to):
        rows = pl.ds(n * (VB // 2), VB // 2)
        return remote(vg.at[block, rows], vg.at[block, rows], vs.at[index], vr.at[index], to)

    first_sends = [hid_half(d, 0, 1, cross), hid_half(d, 1, 2, cross), remote(hx.at[d], hx.at[d], hs.at[0], hr.at[0], part)]
    for k, peer in enumerate(peers):
        first_sends.append(remote(posb.at[d], posb.at[d], ps.at[k], pr.at[k], peer))
        first_sends.append(remote(maskb.at[d], maskb.at[d], ms.at[k], mr.at[k], peer))
    for copy in first_sends:
        copy.start()
    for m in range(4, SP):
        issue(m, m, m + 1)
    vis_part = remote(vg.at[d], vg.at[d], vs.at[0], vr.at[0], part)

    for k, peer in enumerate(peers):
        remote(posb.at[peer], posb.at[peer], ps.at[k], pr.at[k], peer).wait_recv()
        remote(maskb.at[peer], maskb.at[peer], ms.at[k], mr.at[k], peer).wait_recv()

    sign = jnp.where(lax.broadcasted_iota(jnp.int32, (TB, HD), 1) < HD // 2, -1.0, 1.0)
    eye = lax.broadcasted_iota(jnp.int32, (TB, TB), 0) == lax.broadcasted_iota(jnp.int32, (TB, TB), 1)
    freqs = freq[...]

    def as_column(row):
        return jnp.sum(jnp.where(eye, jnp.broadcast_to(row, (TB, TB)), 0.0), axis=1, keepdims=True)

    for block in range(4):
        rows = pl.ds(block * TB, TB)
        angles = as_column(posb[block].astype(F32)) * freqs
        cosb[rows, :] = jnp.cos(angles)
        sinb[rows, :] = jnp.sin(angles) * sign
        seen = (maskb[block] > 0).astype(F32)
        for tile in range(4):
            visb[rows, tile * (V // 4):(tile + 1) * (V // 4)] = jnp.broadcast_to(as_column(seen[tile:tile + 1]), (TB, V // 4))
        keepb[rows, :] = jnp.broadcast_to(as_column(jnp.max(seen, axis=0, keepdims=True)), (TB, HD))

    own_vis.wait()
    for n in range(2):
        hid_half(cross, n, 1 + n, cross).wait_recv()
        hid_half(cross, n, 3 + n, part).start()
    vis_part.start()
    vis_half(d, 0, 1, cross).start()
    remote(hx.at[part], hx.at[part], hs.at[0], hr.at[0], part).wait_recv()
    for n in range(2):
        hid_half(diag, n, 3 + n, part).wait_recv()

    for c in range(D // NC):
        h[c] = hx[:, :, c * NC:(c + 1) * NC].reshape(T, NC)

    def normalise(gain):
        total = jnp.zeros((T, NC), F32)
        for c in range(D // NC):
            v = h[c].astype(F32)
            total = total + v * v
        scale = lax.rsqrt(jnp.sum(total, axis=1, keepdims=True) * (1.0 / D) + NORM_EPS)
        for c in range(D // NC):
            g = gain[pl.ds(c * NC, NC)].astype(F32).reshape(1, NC)
            x[:, c * NC:(c + 1) * NC] = (h[c].astype(F32) * scale * g).astype(BF16)

    def head_norm(v, gain):
        scale = lax.rsqrt(jnp.mean(v * v, axis=1, keepdims=True) + NORM_EPS)
        return v * scale * gain[...].astype(F32).reshape(1, HD)

    def rope(v):
        return v * cosb[...] + pltpu.roll(v, HD // 2, 1) * sinb[...]

    def attend(keys, mask):
        for g in range(KV):
            q = qb[pl.ds(g * REP, REP)].reshape(REP * T, HD)
            scores = dot_t(q, kb[g, pl.ds(0, keys)]) * (HD ** -0.5)
            scores = jnp.where(mask, scores, MASK_VALUE)
            top = jnp.max(scores, axis=1, keepdims=True)
            e = jnp.exp(scores - top)
            p = (e / jnp.sum(e, axis=1, keepdims=True)).astype(BF16)
            o = dot(p, vb[g, pl.ds(0, keys)]).astype(BF16)
            for r in range(REP):
                head = g * REP + r
                ctx[:, head * HD:(head + 1) * HD] = o[r * T:(r + 1) * T]

    def spread(parity, partials, update, between=None):
        def hop1(i):
            return remote(pb.at[1 - core, i], rcv1.at[i], s1.at[i], r1.at[i], part)

        def hop2(i):
            return remote(snd2.at[i], rcv2.at[parity, i], s2.at[parity, i], r2.at[parity, i], cross)

        def hop3(half, i):
            return remote(h.at[half * 8 + i], h.at[half * 8 + i], s3.at[i], r3.at[i], part)

        def fold(i):
            hop1(i).wait_recv()
            snd2[i] = (pb[core, i].astype(F32) + rcv1[i].astype(F32)).astype(BF16)
            hop2(i).start()

        def step(j, carry):
            for n, (low, high) in enumerate(partials(j)):
                i = 2 * j + n
                pb[0, i] = low.astype(BF16)
                pb[1, i] = high.astype(BF16)
                hop1(i).start()

            @pl.when(j >= 1)
            def _():
                fold(2 * j - 2)
                fold(2 * j - 1)
            return carry

        lax.fori_loop(0, 4, step, 0)
        fold(6)
        fold(7)
        if between is not None:
            between()

        def final(i, carry):
            hop2(i).wait_recv()
            total = snd2[i].astype(F32) + rcv2[parity, i].astype(F32)
            mine = core * 8 + i
            h[mine] = (h[mine].astype(F32) + update(total)).astype(BF16)
            hop3(core, i).start()
            return carry

        lax.fori_loop(0, 8, final, 0)

        def finish(i, carry):
            hop3(1 - core, i).wait_recv()
            hop3(core, i).wait_send()
            hop1(i).wait_send()
            hop2(i).wait_send()
            return carry

        lax.fori_loop(0, 8, finish, 0)

    def wo_partials(base):
        def partials(j):
            m = base + j // 2
            slot = lax.rem(m, SP)

            @pl.when(lax.rem(j, 2) == 0)
            def _():
                arrive(m)
            out = []
            for n in range(2):
                rows = pl.ds(pl.multiple_of((lax.rem(j, 2) * 2 + n) * WO_ROWS, WO_ROWS), WO_ROWS)
                out.append((dot(ctx[...], wbuf[slot, 0, rows]), dot(ctx[...], wbuf[slot, 1, rows])))

            @pl.when(lax.rem(j, 2) == 1)
            def _():
                refill(m, base, base + 2)
            return out
        return partials

    def wd_partials(base):
        def partials(j):
            slots = [arrive(base + 2 * j + n, FF) for n in range(2)]
            out = []
            for slot in slots:
                rows = pl.ds(0, FF)
                out.append((dot(act[...], wbuf[slot, 0, rows]), dot(act[...], wbuf[slot, 1, rows])))
            for n in range(2):
                refill(base + 2 * j + n, base, base + 8)
            return out
        return partials

    def mlp_up(base):
        def step(i, carry):
            slots = [arrive(base + 2 * i + n) for n in range(2)]
            for n, slot in enumerate(slots):
                gate = dot(x[...], wbuf[slot, 0])
                up = dot(x[...], wbuf[slot, 1])
                act[:, cols(2 * i + n)] = (gate * jax.nn.sigmoid(gate) * up).astype(BF16)
            for n in range(2):
                refill(base + 2 * i + n, base, base + 14)
            return carry
        lax.fori_loop(0, 7, step, 0)

    def queries(base, finish):
        slots = [arrive(base + i) for i in range(2)]
        for i, slot in enumerate(slots):
            for half in range(2):
                q = dot(x[...], wbuf[slot, half])
                for sub in range(2):
                    qb[4 * i + 2 * half + sub] = finish(q[:, sub * HD:(sub + 1) * HD]).astype(BF16)

    normalise(ln1a)
    slot_kv = arrive(BASE['kva'])
    queries(BASE['qa'], rope)
    keys, vals = dot(x[...], wbuf[slot_kv, 0]), dot(x[...], wbuf[slot_kv, 1])
    for g in range(KV):
        kb[g, pl.ds(0, T)] = rope(keys[:, g * HD:(g + 1) * HD]).astype(BF16)
        vb[g, pl.ds(0, T)] = vals[:, g * HD:(g + 1) * HD].astype(BF16)
    for m in range(3):
        refill(m, m, m + 1)
    query_at = lax.rem(lax.broadcasted_iota(jnp.int32, (REP * T, T), 0), T)
    attend(T, query_at >= lax.broadcasted_iota(jnp.int32, (REP * T, T), 1))
    spread(0, wo_partials(BASE['oa']), lambda total: total)
    vis_half(d, 1, 2, cross).start()
    normalise(ln2a)
    mlp_up(BASE['gua'])
    for n in range(2):
        vis_half(cross, n, 1 + n, cross).wait_recv()
        vis_half(cross, n, 3 + n, part).start()

    def vision_heads():
        remote(vg.at[part], vg.at[part], vs.at[0], vr.at[0], part).wait_recv()
        for n in range(2):
            vis_half(diag, n, 3 + n, part).wait_recv()
        slot = arrive(BASE['kvb'])

        def kv_step(n, carry):
            rows = pl.ds(pl.multiple_of(n * 2 * VB, 2 * VB), 2 * VB)
            lhs = vg[pl.ds(2 * n, 2)].reshape(2 * VB, D)
            keys = dot(lhs, wbuf[slot, 0])
            vals = dot(lhs, wbuf[slot, 1])
            for g in range(KV):
                kb[g, rows] = head_norm(keys[:, g * HD:(g + 1) * HD], kn).astype(BF16)
                vb[g, rows] = vals[:, g * HD:(g + 1) * HD].astype(BF16)
            return carry

        lax.fori_loop(0, 2, kv_step, 0)
        refill(BASE['kvb'], BASE['kvb'], BASE['kvb'] + 1)

    spread(1, wd_partials(BASE['da']), lambda total: total, vision_heads)

    normalise(ln1b)
    queries(BASE['qb'], lambda q: head_norm(q, qn))
    for i in range(2):
        refill(BASE['qb'] + i, BASE['qb'] + i, BASE['qb'] + i + 1)
    attend(V, jnp.concatenate([visb[...]] * REP, axis=0) > 0.0)
    gate0 = jnp.tanh(jnp.full((T, 1), xg[0], F32)) * keepb[:, 0:1]
    spread(2, wo_partials(BASE['ob']), lambda total: gate0 * total)
    normalise(ln2b)
    mlp_up(BASE['gub'])

    own = pl.ds(pl.multiple_of(d * TB, TB), TB)
    gate1 = jnp.tanh(jnp.full((TB, 1), xg[1], F32)) * keepb[own, 0:1]
    down = wd_partials(BASE['db'])

    def last_step(j, carry):
        for n, values in enumerate(down(j)):
            i = 2 * j + n
            for half, value in enumerate(values):
                pf[i, :, half] = value.astype(BF16).reshape(4, TB, NC)
            for k, peer in enumerate(peers):
                remote(pf.at[i, peer], rcvf.at[i, k], fs.at[i, k], fr.at[i, k], peer).start()
        return carry

    lax.fori_loop(0, 4, last_step, 0)

    def last_sum(i, carry):
        for k, peer in enumerate(peers):
            remote(pf.at[i, peer], rcvf.at[i, k], fs.at[i, k], fr.at[i, k], peer).wait_recv()
        for half in range(2):
            total = pf[i, d, half].astype(F32)
            for k in range(3):
                total = total + rcvf[i, k, half].astype(F32)
            chunk = i + 8 * half
            obuf[:, cols(chunk)] = (h[chunk, own].astype(F32) + gate1 * total).astype(BF16)
            pltpu.make_async_copy(obuf.at[:, cols(chunk)], out.at[0, :, cols(chunk)], osem.at[i, half]).start()
        return carry

    lax.fori_loop(0, 8, last_sum, 0)

    for copy in first_sends:
        copy.wait_send()
    vis_part.wait_send()
    for n in range(2):
        hid_half(cross, n, 3 + n, part).wait_send()
        vis_half(d, n, 1 + n, cross).wait_send()
        vis_half(cross, n, 3 + n, part).wait_send()

    def drain(j, carry):
        for half in range(2):
            piece = cols(j + 8 * half)
            pltpu.make_async_copy(obuf.at[:, piece], out.at[0, :, piece], osem.at[j, half]).wait()
        for k, peer in enumerate(peers):
            remote(pf.at[j, peer], rcvf.at[j, k], fs.at[j, k], fr.at[j, k], peer).wait_send()
        return carry

    lax.fori_loop(0, 8, drain, 0)


def solution(mesh):
    act_spec = P('dp', 'tp', None)
    col_spec = P(None, 'tp')
    row_spec = P('tp', None)
    layer_a = (P(), col_spec, col_spec, col_spec, row_spec, P(), col_spec, col_spec, row_spec)
    layer_b = (P(), col_spec, P(), col_spec, col_spec, P(), row_spec, P(), col_spec, col_spec, row_spec, P())
    in_specs = (act_spec, act_spec, P('dp', 'tp'), act_spec) + layer_a + layer_b
    table = rope_table(HD)

    hbm = pl.BlockSpec(memory_space=pl.ANY)
    vmem = pl.BlockSpec(memory_space=pltpu.VMEM)
    smem = pl.BlockSpec(memory_space=pltpu.SMEM)
    dma = pltpu.SemaphoreType.DMA
    scratch = [
        pltpu.VMEM((SP, 2, D, NC), BF16), dma((SP, 2)),
        pltpu.VMEM((4, TB, D), BF16),
        pltpu.VMEM((4, 1, TB), jnp.int32),
        pltpu.VMEM((4, 4, TB), jnp.int32),
        pltpu.VMEM((T, HD), F32), pltpu.VMEM((T, HD), F32),
        pltpu.VMEM((T, V), F32), pltpu.VMEM((T, HD), F32),
        pltpu.VMEM((D // NC, T, NC), BF16),
        pltpu.VMEM((T, D), BF16),
        pltpu.VMEM((T, FF), BF16),
        pltpu.VMEM((T, WO_ROWS), BF16),
        pltpu.VMEM((KV * REP, T, HD), BF16),
        pltpu.VMEM((KV, V, HD), BF16), pltpu.VMEM((KV, V, HD), BF16),
        pltpu.VMEM((4, VB, D), BF16),
        pltpu.VMEM((2, 8, T, NC), BF16),
        pltpu.VMEM((8, T, NC), BF16),
        pltpu.VMEM((8, T, NC), BF16),
        pltpu.VMEM((3, 8, T, NC), BF16),
        pltpu.VMEM((8, 4, 2, TB, NC), BF16),
        pltpu.VMEM((8, 3, 2, TB, NC), BF16),
        pltpu.VMEM((TB, D), BF16), dma((8, 2)),
        dma((4,)),
        dma((5,)), dma((5,)), dma((3,)), dma((3,)), dma((3,)), dma((3,)),
        dma((5,)), dma((5,)),
        dma((8,)), dma((8,)), dma((3, 8)), dma((3, 8)), dma((8,)), dma((8,)),
        dma((8, 3)), dma((8, 3)),
    ]

    def body(hidden, vision, positions, tile_mask, *params):
        freqs = jnp.asarray(np.concatenate([table, table])[None])
        specs = [hbm, hbm, hbm, hbm, vmem]
        for k, p in enumerate(params):
            specs.append(vmem if p.ndim == 1 else hbm)
        specs[-1] = smem
        return pl.pallas_call(
            kernel,
            out_shape=jax.ShapeDtypeStruct(hidden.shape, BF16),
            in_specs=specs,
            out_specs=hbm,
            scratch_shapes=scratch,
            compiler_params=pltpu.CompilerParams(
                collective_id=0, has_side_effects=True, vmem_limit_bytes=67043328),
            cost_estimate=pl.CostEstimate(flops=2 * 64 * 109051904, bytes_accessed=218103808, transcendentals=0),
            name='layers',
        )(hidden, vision, positions, jnp.swapaxes(tile_mask, 1, 2), freqs, *params)

    return jax.shard_map(body, mesh=mesh, in_specs=in_specs, out_specs=act_spec, check_vma=False)
```

```python
import math
import jax
import jax.numpy as jnp
import numpy as np
from jax import lax
from jax.experimental import pallas as pl
from jax.experimental.pallas import tpu as pltpu
from jax.sharding import PartitionSpec as P

ROPE_THETA = 500000.0
ROPE_FACTOR = 8.0
LOW_FACTOR = 1.0
HIGH_FACTOR = 4.0
ORIG_CONTEXT = 8192.0
NORM_EPS = 1e-5
MASK_VALUE = -1e30
MESH = pl.DeviceIdType.MESH
BF16 = jnp.bfloat16
F32 = jnp.float32

T = 64
TB = 16
D = 4096
V = 256
VB = 64
HD = 128
KV = 2
REP = 4
FF = 3584
NC = 256
SP = 13
EARLY = 6
WO_ROWS = KV * REP * HD

SEGMENTS = []
_at = 0
for _name, _count in (('qa', 2), ('kva', 1), ('oa', 2), ('gua', 14), ('da', 8),
                      ('kvb', 1), ('qb', 2), ('ob', 2), ('gub', 14), ('db', 8)):
    SEGMENTS.append((_name, _at, _count))
    _at += _count
TOTAL = _at
BASE = {name: first for name, first, _ in SEGMENTS}


def rope_table(head_dim):
    low_wave = ORIG_CONTEXT / LOW_FACTOR
    high_wave = ORIG_CONTEXT / HIGH_FACTOR
    freq_list = []
    for freq_idx in range(head_dim // 2):
        base_freq = 1.0 / (ROPE_THETA ** (2.0 * freq_idx / head_dim))
        wave_len = 2.0 * math.pi / base_freq
        if wave_len > low_wave:
            freq_list.append(base_freq / ROPE_FACTOR)
        elif wave_len < high_wave:
            freq_list.append(base_freq)
        else:
            smooth = (ORIG_CONTEXT / wave_len - LOW_FACTOR) / (HIGH_FACTOR - LOW_FACTOR)
            freq_list.append((1.0 - smooth) * base_freq / ROPE_FACTOR + smooth * base_freq)
    return np.array(freq_list, dtype=np.float32)


def dot(a, b):
    return jnp.dot(a, b, preferred_element_type=F32)


def dot_t(a, b):
    return lax.dot_general(a, b, (((1,), (1,)), ((), ())), preferred_element_type=F32)


def kernel(hid, vis, pos, tmask, freq,
           ln1a, wqa, wka, wva, woa, ln2a, wga, wua, wda,
           ln1b, wqb, qn, wkb, wvb, kn, wob, ln2b, wgb, wub, wdb, xg,
           out,
           wbuf, wsem, hx, posb, maskb, cosb, sinb, visb, keepb, h, x, act, ctx, qb, kb, vb, vg,
           pb, rcv1, snd2, rcv2, pf, rcvf, obuf, osem, gbuf, ssq, rbuf, acc,
           lsem, hs, hr, ps, pr, ms, mr, vs, vr, s1, r1, s2, r2, s3, r3, fs, fr):
    d = lax.axis_index('tp')
    core = lax.rem(d, 2)
    part = d + 1 - 2 * core
    cross = lax.rem(d + 2, 4)
    diag = 3 - d
    peers = (part, cross, diag)
    weights = {
        'qa': (wqa,), 'kva': (wka, wva), 'oa': (woa,), 'gua': (wga, wua), 'da': (wda,),
        'qb': (wqb,), 'kvb': (wkb, wvb), 'ob': (wob,), 'gub': (wgb, wub), 'db': (wdb,),
    }

    def cols(index):
        return pl.ds(pl.multiple_of(index * NC, NC), NC)

    def start_segment(name, first, m):
        slot = lax.rem(m, SP)
        i = m - first
        refs = weights[name]
        kind = name[:-1]
        if kind == 'q':
            for half in range(2):
                pltpu.make_async_copy(refs[0].at[:, cols(2 * i + half)], wbuf.at[slot, half], wsem.at[slot, half]).start()
        elif kind == 'kv':
            for half in range(2):
                pltpu.make_async_copy(refs[half], wbuf.at[slot, half], wsem.at[slot, half]).start()
        elif kind == 'gu':
            for half in range(2):
                pltpu.make_async_copy(refs[half].at[:, cols(i)], wbuf.at[slot, half], wsem.at[slot, half]).start()
        elif kind == 'd':
            for half in range(2):
                pltpu.make_async_copy(refs[0].at[:, cols(i + 8 * half)], wbuf.at[slot, half, pl.ds(0, FF)], wsem.at[slot, half]).start()
        else:
            for half in range(2):
                for sub in range(4):
                    pltpu.make_async_copy(refs[0].at[:, cols(4 * i + sub + 8 * half)],
                                          wbuf.at[slot, half, pl.ds(sub * WO_ROWS, WO_ROWS)], wsem.at[slot, half]).start()

    def issue(m, low, high):
        for name, first, count in SEGMENTS:
            if first >= high or first + count <= low:
                continue
            if first <= low and high <= first + count:
                start_segment(name, first, m)
            else:
                @pl.when(jnp.logical_and(m >= first, m < first + count))
                def _():
                    start_segment(name, first, m)

    def refill(m, low, high):
        if low + SP < TOTAL:
            issue(m + SP, low + SP, high + SP)

    def arrive(m, rows=D):
        slot = lax.rem(m, SP)
        for half in range(2):
            dst = wbuf.at[slot, half, pl.ds(0, rows)]
            pltpu.make_async_copy(dst, dst, wsem.at[slot, half]).wait()
        return slot

    def remote(src, dst, send, recv, to):
        return pltpu.make_async_remote_copy(src_ref=src, dst_ref=dst, send_sem=send, recv_sem=recv,
                                            device_id={'tp': to}, device_id_type=MESH)

    own_rows = pltpu.make_async_copy(hid.at[0], hx.at[d], lsem.at[0])
    own_rows.start()
    own_pos = pltpu.make_async_copy(pos, posb.at[d], lsem.at[1])
    own_pos.start()
    own_mask = pltpu.make_async_copy(tmask.at[0], maskb.at[d], lsem.at[2])
    own_mask.start()
    own_vis = pltpu.make_async_copy(vis.at[0], vg.at[d], lsem.at[3])
    own_vis.start()
    barrier = pltpu.get_barrier_semaphore()
    for peer in peers:
        pl.semaphore_signal(barrier, inc=1, device_id={'tp': peer}, device_id_type=MESH)
    for m in range(4):
        issue(m, m, m + 1)
    own_rows.wait()
    own_pos.wait()
    own_mask.wait()
    pl.semaphore_wait(barrier, 3)

    def hid_half(block, n, index, to):
        rows = pl.ds(n * (TB // 2), TB // 2)
        return remote(hx.at[block, rows], hx.at[block, rows], hs.at[index], hr.at[index], to)

    def vis_half(block, n, index, to):
        rows = pl.ds(n * (VB // 2), VB // 2)
        return remote(vg.at[block, rows], vg.at[block, rows], vs.at[index], vr.at[index], to)

    first_sends = [hid_half(d, 0, 1, cross), hid_half(d, 1, 2, cross), remote(hx.at[d], hx.at[d], hs.at[0], hr.at[0], part)]
    for k, peer in enumerate(peers):
        first_sends.append(remote(posb.at[d], posb.at[d], ps.at[k], pr.at[k], peer))
        first_sends.append(remote(maskb.at[d], maskb.at[d], ms.at[k], mr.at[k], peer))
    for copy in first_sends:
        copy.start()
    for m in range(4, SP):
        issue(m, m, m + 1)
    vis_part = remote(vg.at[d], vg.at[d], vs.at[0], vr.at[0], part)

    for k, peer in enumerate(peers):
        remote(posb.at[peer], posb.at[peer], ps.at[k], pr.at[k], peer).wait_recv()
        remote(maskb.at[peer], maskb.at[peer], ms.at[k], mr.at[k], peer).wait_recv()

    sign = jnp.where(lax.broadcasted_iota(jnp.int32, (TB, HD), 1) < HD // 2, -1.0, 1.0)
    eye = lax.broadcasted_iota(jnp.int32, (TB, TB), 0) == lax.broadcasted_iota(jnp.int32, (TB, TB), 1)
    freqs = freq[...]

    def as_column(row):
        return jnp.sum(jnp.where(eye, jnp.broadcast_to(row, (TB, TB)), 0.0), axis=1, keepdims=True)

    for block in range(4):
        rows = pl.ds(block * TB, TB)
        angles = as_column(posb[block].astype(F32)) * freqs
        cosb[rows, :] = jnp.cos(angles)
        sinb[rows, :] = jnp.sin(angles) * sign
        seen = (maskb[block] > 0).astype(F32)
        for tile in range(4):
            visb[rows, tile * (V // 4):(tile + 1) * (V // 4)] = jnp.broadcast_to(as_column(seen[tile:tile + 1]), (TB, V // 4))
        keepb[rows, :] = jnp.broadcast_to(as_column(jnp.max(seen, axis=0, keepdims=True)), (TB, HD))

    for k, gain in enumerate((ln1a, ln2a, ln1b, ln2b)):
        for c in range(D // NC):
            gbuf[k, c] = gain[pl.ds(c * NC, NC)].astype(F32).reshape(1, NC)
    own_vis.wait()
    for n in range(2):
        hid_half(cross, n, 1 + n, cross).wait_recv()
        hid_half(cross, n, 3 + n, part).start()
    vis_part.start()
    vis_half(d, 0, 1, cross).start()
    remote(hx.at[part], hx.at[part], hs.at[0], hr.at[0], part).wait_recv()
    for n in range(2):
        hid_half(diag, n, 3 + n, part).wait_recv()

    def take(c, value, gain):
        v = value.astype(F32)
        x[:, cols(c)] = (v * gbuf[gain, c]).astype(BF16)
        ssq[...] += v * v

    def row_scale():
        scale = lax.rsqrt(jnp.sum(ssq[...], axis=1, keepdims=True) * (1.0 / D) + NORM_EPS)
        rbuf[...] = jnp.broadcast_to(scale, (T, HD))

    ssq[...] = jnp.zeros((T, NC), F32)
    for c in range(D // NC):
        h[c] = hx[:, :, c * NC:(c + 1) * NC].reshape(T, NC)
        take(c, h[c], 0)
    row_scale()

    def head_norm(v, gain):
        scale = lax.rsqrt(jnp.mean(v * v, axis=1, keepdims=True) + NORM_EPS)
        return v * scale * gain[...].astype(F32).reshape(1, HD)

    def rope(v):
        return v * cosb[...] + pltpu.roll(v, HD // 2, 1) * sinb[...]

    def attend(keys, mask):
        for g in range(KV):
            q = qb[pl.ds(g * REP, REP)].reshape(REP * T, HD)
            scores = dot_t(q, kb[g, pl.ds(0, keys)]) * (HD ** -0.5)
            scores = jnp.where(mask, scores, MASK_VALUE)
            top = jnp.max(scores, axis=1, keepdims=True)
            e = jnp.exp(scores - top)
            p = (e / jnp.sum(e, axis=1, keepdims=True)).astype(BF16)
            o = dot(p, vb[g, pl.ds(0, keys)]).astype(BF16)
            for r in range(REP):
                head = g * REP + r
                ctx[:, head * HD:(head + 1) * HD] = o[r * T:(r + 1) * T]

    def spread(parity, partials, update, gain, first, count, between=None):
        def hop1(i):
            return remote(pb.at[1 - core, i], rcv1.at[i], s1.at[i], r1.at[i], part)

        def hop2(i):
            return remote(snd2.at[i], rcv2.at[parity, i], s2.at[parity, i], r2.at[parity, i], cross)

        def hop3(half, i):
            return remote(h.at[half * 8 + i], h.at[half * 8 + i], s3.at[i], r3.at[i], part)

        def fold(i):
            hop1(i).wait_recv()
            snd2[i] = (pb[core, i].astype(F32) + rcv1[i].astype(F32)).astype(BF16)
            hop2(i).start()

        def step(j, carry):
            for n, (low, high) in enumerate(partials(j)):
                i = 2 * j + n
                pb[0, i] = low.astype(BF16)
                pb[1, i] = high.astype(BF16)
                hop1(i).start()

            @pl.when(j >= 1)
            def _():
                fold(2 * j - 2)
                fold(2 * j - 1)
            return carry

        lax.fori_loop(0, 4, step, 0)
        fold(6)
        fold(7)
        if between is not None:
            between()

        def final(i):
            hop2(i).wait_recv()
            total = snd2[i].astype(F32) + rcv2[parity, i].astype(F32)
            mine = core * 8 + i
            value = (h[mine].astype(F32) + update(total)).astype(BF16)
            h[mine] = value
            hop3(core, i).start()
            take(mine, value, gain)

        ssq[...] = jnp.zeros((T, NC), F32)
        for e in range(count):
            for half in range(2):
                acc[e, half] = jnp.zeros((T, NC), F32)
            arrive(first + e)
        final(0)
        final(1)

        def stage(n, carry):
            @pl.when(n < 3)
            def _():
                final(2 * n + 2)
                final(2 * n + 3)
            for k in range(2):
                i = 2 * n + k
                theirs = (1 - core) * 8 + i
                hop3(1 - core, i).wait_recv()
                take(theirs, h[theirs], gain)
            low = pl.ds(pl.multiple_of(n * 2 * NC, 2 * NC), 2 * NC)
            high = pl.ds(pl.multiple_of(n * 2 * NC + D // 2, 2 * NC), 2 * NC)
            x_low, x_high = x[:, low], x[:, high]
            for e in range(count):
                slot = (first + e) % SP
                for half in range(2):
                    acc[e, half] += dot(x_low, wbuf[slot, half, low]) + dot(x_high, wbuf[slot, half, high])
            return carry

        lax.fori_loop(0, 4, stage, 0)
        row_scale()

        def finish(i, carry):
            hop3(core, i).wait_send()
            hop1(i).wait_send()
            hop2(i).wait_send()
            return carry

        lax.fori_loop(0, 8, finish, 0)

    def wo_partials(base):
        def partials(j):
            m = base + j // 2
            slot = lax.rem(m, SP)

            @pl.when(lax.rem(j, 2) == 0)
            def _():
                arrive(m)
            out = []
            for n in range(2):
                rows = pl.ds(pl.multiple_of((lax.rem(j, 2) * 2 + n) * WO_ROWS, WO_ROWS), WO_ROWS)
                out.append((dot(ctx[...], wbuf[slot, 0, rows]), dot(ctx[...], wbuf[slot, 1, rows])))

            @pl.when(lax.rem(j, 2) == 1)
            def _():
                refill(m, base, base + 2)
            return out
        return partials

    def wd_partials(base):
        def partials(j):
            slots = [arrive(base + 2 * j + n, FF) for n in range(2)]
            out = []
            for slot in slots:
                rows = pl.ds(0, FF)
                out.append((dot(act[...], wbuf[slot, 0, rows]), dot(act[...], wbuf[slot, 1, rows])))
            for n in range(2):
                refill(base + 2 * j + n, base, base + 8)
            return out
        return partials

    def mlp_up(base):
        def activate(i, gate, up):
            gate = gate * rbuf[:, 0:1]
            act[:, cols(i)] = (gate * jax.nn.sigmoid(gate) * (up * rbuf[:, 0:1])).astype(BF16)

        for e in range(EARLY):
            activate(e, acc[e, 0], acc[e, 1])
            refill(base + e, base + e, base + e + 1)

        def step(i, carry):
            slots = [arrive(base + 2 * i + n) for n in range(2)]
            for n, slot in enumerate(slots):
                activate(2 * i + n, dot(x[...], wbuf[slot, 0]), dot(x[...], wbuf[slot, 1]))
            for n in range(2):
                refill(base + 2 * i + n, base + EARLY, base + 14)
            return carry
        lax.fori_loop(EARLY // 2, 7, step, 0)

    def queries(products, finish):
        for n, q in enumerate(products):
            q = q * rbuf[:, 0:1]
            for sub in range(2):
                qb[2 * n + sub] = finish(q[:, sub * HD:(sub + 1) * HD]).astype(BF16)

    slots_a = [arrive(m) for m in range(3)]
    queries([dot(x[...], wbuf[slot, half]) for slot in slots_a[:2] for half in range(2)], rope)
    keys, vals = [dot(x[...], wbuf[slots_a[2], half]) * rbuf[:, 0:1] for half in range(2)]
    for g in range(KV):
        kb[g, pl.ds(0, T)] = rope(keys[:, g * HD:(g + 1) * HD]).astype(BF16)
        vb[g, pl.ds(0, T)] = vals[:, g * HD:(g + 1) * HD].astype(BF16)
    for m in range(3):
        refill(m, m, m + 1)
    query_at = lax.rem(lax.broadcasted_iota(jnp.int32, (REP * T, T), 0), T)
    attend(T, query_at >= lax.broadcasted_iota(jnp.int32, (REP * T, T), 1))

    def vision_send():
        vis_half(d, 1, 2, cross).start()

    spread(0, wo_partials(BASE['oa']), lambda total: total, 1, BASE['gua'], EARLY, vision_send)
    mlp_up(BASE['gua'])
    down_a = wd_partials(BASE['da'])

    def down_and_forward(j):
        @pl.when(j == 1)
        def _():
            for n in range(2):
                vis_half(cross, n, 1 + n, cross).wait_recv()
                vis_half(cross, n, 3 + n, part).start()
        return down_a(j)

    def vision_heads():
        remote(vg.at[part], vg.at[part], vs.at[0], vr.at[0], part).wait_recv()
        for n in range(2):
            vis_half(diag, n, 3 + n, part).wait_recv()
        slot = arrive(BASE['kvb'])

        def kv_step(n, carry):
            rows = pl.ds(pl.multiple_of(n * 2 * VB, 2 * VB), 2 * VB)
            lhs = vg[pl.ds(2 * n, 2)].reshape(2 * VB, D)
            keys = dot(lhs, wbuf[slot, 0])
            vals = dot(lhs, wbuf[slot, 1])
            for g in range(KV):
                kb[g, rows] = head_norm(keys[:, g * HD:(g + 1) * HD], kn).astype(BF16)
                vb[g, rows] = vals[:, g * HD:(g + 1) * HD].astype(BF16)
            return carry

        lax.fori_loop(0, 2, kv_step, 0)
        refill(BASE['kvb'], BASE['kvb'], BASE['kvb'] + 1)

    spread(1, down_and_forward, lambda total: total, 2, BASE['qb'], 2, vision_heads)

    queries([acc[e, half] for e in range(2) for half in range(2)], lambda q: head_norm(q, qn))
    for i in range(2):
        refill(BASE['qb'] + i, BASE['qb'] + i, BASE['qb'] + i + 1)
    attend(V, jnp.concatenate([visb[...]] * REP, axis=0) > 0.0)
    gate0 = jnp.tanh(jnp.full((T, 1), xg[0], F32)) * keepb[:, 0:1]
    spread(2, wo_partials(BASE['ob']), lambda total: gate0 * total, 3, BASE['gub'], EARLY)
    mlp_up(BASE['gub'])

    own = pl.ds(pl.multiple_of(d * TB, TB), TB)
    gate1 = jnp.tanh(jnp.full((TB, 1), xg[1], F32)) * keepb[own, 0:1]
    down = wd_partials(BASE['db'])

    def last_step(j, carry):
        for n, values in enumerate(down(j)):
            i = 2 * j + n
            for half, value in enumerate(values):
                pf[i, :, half] = value.astype(BF16).reshape(4, TB, NC)
            for k, peer in enumerate(peers):
                remote(pf.at[i, peer], rcvf.at[i, k], fs.at[i, k], fr.at[i, k], peer).start()
        return carry

    lax.fori_loop(0, 4, last_step, 0)

    def last_sum(i, carry):
        for k, peer in enumerate(peers):
            remote(pf.at[i, peer], rcvf.at[i, k], fs.at[i, k], fr.at[i, k], peer).wait_recv()
        for half in range(2):
            total = pf[i, d, half].astype(F32)
            for k in range(3):
                total = total + rcvf[i, k, half].astype(F32)
            chunk = i + 8 * half
            obuf[:, cols(chunk)] = (h[chunk, own].astype(F32) + gate1 * total).astype(BF16)
            pltpu.make_async_copy(obuf.at[:, cols(chunk)], out.at[0, :, cols(chunk)], osem.at[i, half]).start()
        return carry

    lax.fori_loop(0, 8, last_sum, 0)

    for copy in first_sends:
        copy.wait_send()
    vis_part.wait_send()
    for n in range(2):
        hid_half(cross, n, 3 + n, part).wait_send()
        vis_half(d, n, 1 + n, cross).wait_send()
        vis_half(cross, n, 3 + n, part).wait_send()

    def drain(j, carry):
        for half in range(2):
            piece = cols(j + 8 * half)
            pltpu.make_async_copy(obuf.at[:, piece], out.at[0, :, piece], osem.at[j, half]).wait()
        for k, peer in enumerate(peers):
            remote(pf.at[j, peer], rcvf.at[j, k], fs.at[j, k], fr.at[j, k], peer).wait_send()
        return carry

    lax.fori_loop(0, 8, drain, 0)


def solution(mesh):
    act_spec = P('dp', 'tp', None)
    col_spec = P(None, 'tp')
    row_spec = P('tp', None)
    layer_a = (P(), col_spec, col_spec, col_spec, row_spec, P(), col_spec, col_spec, row_spec)
    layer_b = (P(), col_spec, P(), col_spec, col_spec, P(), row_spec, P(), col_spec, col_spec, row_spec, P())
    in_specs = (act_spec, act_spec, P('dp', 'tp'), act_spec) + layer_a + layer_b
    table = rope_table(HD)

    hbm = pl.BlockSpec(memory_space=pl.ANY)
    vmem = pl.BlockSpec(memory_space=pltpu.VMEM)
    smem = pl.BlockSpec(memory_space=pltpu.SMEM)
    dma = pltpu.SemaphoreType.DMA
    scratch = [
        pltpu.VMEM((SP, 2, D, NC), BF16), dma((SP, 2)),
        pltpu.VMEM((4, TB, D), BF16),
        pltpu.VMEM((4, 1, TB), jnp.int32),
        pltpu.VMEM((4, 4, TB), jnp.int32),
        pltpu.VMEM((T, HD), F32), pltpu.VMEM((T, HD), F32),
        pltpu.VMEM((T, V), F32), pltpu.VMEM((T, HD), F32),
        pltpu.VMEM((D // NC, T, NC), BF16),
        pltpu.VMEM((T, D), BF16),
        pltpu.VMEM((T, FF), BF16),
        pltpu.VMEM((T, WO_ROWS), BF16),
        pltpu.VMEM((KV * REP, T, HD), BF16),
        pltpu.VMEM((KV, V, HD), BF16), pltpu.VMEM((KV, V, HD), BF16),
        pltpu.VMEM((4, VB, D), BF16),
        pltpu.VMEM((2, 8, T, NC), BF16),
        pltpu.VMEM((8, T, NC), BF16),
        pltpu.VMEM((8, T, NC), BF16),
        pltpu.VMEM((3, 8, T, NC), BF16),
        pltpu.VMEM((8, 4, 2, TB, NC), BF16),
        pltpu.VMEM((8, 3, 2, TB, NC), BF16),
        pltpu.VMEM((TB, D), BF16), dma((8, 2)),
        pltpu.VMEM((4, D // NC, 1, NC), F32), pltpu.VMEM((T, NC), F32), pltpu.VMEM((T, HD), F32),
        pltpu.VMEM((EARLY, 2, T, NC), F32),
        dma((4,)),
        dma((5,)), dma((5,)), dma((3,)), dma((3,)), dma((3,)), dma((3,)),
        dma((5,)), dma((5,)),
        dma((8,)), dma((8,)), dma((3, 8)), dma((3, 8)), dma((8,)), dma((8,)),
        dma((8, 3)), dma((8, 3)),
    ]

    def body(hidden, vision, positions, tile_mask, *params):
        freqs = jnp.asarray(np.concatenate([table, table])[None])
        specs = [hbm, hbm, hbm, hbm, vmem]
        for k, p in enumerate(params):
            specs.append(vmem if p.ndim == 1 else hbm)
        specs[-1] = smem
        return pl.pallas_call(
            kernel,
            out_shape=jax.ShapeDtypeStruct(hidden.shape, BF16),
            in_specs=specs,
            out_specs=hbm,
            scratch_shapes=scratch,
            compiler_params=pltpu.CompilerParams(
                collective_id=0, has_side_effects=True, vmem_limit_bytes=67043328),
            cost_estimate=pl.CostEstimate(flops=2 * 64 * 109051904, bytes_accessed=218103808, transcendentals=0),
            name='layers',
        )(hidden, vision, positions, jnp.swapaxes(tile_mask, 1, 2), freqs, *params)

    return jax.shard_map(body, mesh=mesh, in_specs=in_specs, out_specs=act_spec, check_vma=False)
```

```python
import math
import jax
import jax.numpy as jnp
import numpy as np
from jax import lax
from jax.experimental import pallas as pl
from jax.experimental.pallas import tpu as pltpu
from jax.sharding import PartitionSpec as P

ROPE_THETA = 500000.0
ROPE_FACTOR = 8.0
LOW_FACTOR = 1.0
HIGH_FACTOR = 4.0
ORIG_CONTEXT = 8192.0
NORM_EPS = 1e-5
MASK_VALUE = -1e30
MESH = pl.DeviceIdType.MESH
BF16 = jnp.bfloat16
F32 = jnp.float32

T = 64
TB = 16
D = 4096
V = 256
VB = 64
HD = 128
KV = 2
REP = 4
FF = 3584
NC = 256
SP = 13
EARLY = 6
WO_ROWS = KV * REP * HD

SEGMENTS = []
_at = 0
for _name, _count in (('qa', 2), ('kva', 1), ('oa', 2), ('gua', 14), ('da', 8),
                      ('kvb', 1), ('qb', 2), ('ob', 2), ('gub', 14), ('db', 8)):
    SEGMENTS.append((_name, _at, _count))
    _at += _count
TOTAL = _at
BASE = {name: first for name, first, _ in SEGMENTS}


def rope_table(head_dim):
    low_wave = ORIG_CONTEXT / LOW_FACTOR
    high_wave = ORIG_CONTEXT / HIGH_FACTOR
    freq_list = []
    for freq_idx in range(head_dim // 2):
        base_freq = 1.0 / (ROPE_THETA ** (2.0 * freq_idx / head_dim))
        wave_len = 2.0 * math.pi / base_freq
        if wave_len > low_wave:
            freq_list.append(base_freq / ROPE_FACTOR)
        elif wave_len < high_wave:
            freq_list.append(base_freq)
        else:
            smooth = (ORIG_CONTEXT / wave_len - LOW_FACTOR) / (HIGH_FACTOR - LOW_FACTOR)
            freq_list.append((1.0 - smooth) * base_freq / ROPE_FACTOR + smooth * base_freq)
    return np.array(freq_list, dtype=np.float32)


def dot(a, b):
    return jnp.dot(a, b, preferred_element_type=F32)


def dot_t(a, b):
    return lax.dot_general(a, b, (((1,), (1,)), ((), ())), preferred_element_type=F32)


def kernel(hid, vis, pos, tmask, freq_hbm,
           ln1a_hbm, wqa, wka, wva, woa, ln2a_hbm, wga, wua, wda,
           ln1b_hbm, wqb, qn_hbm, wkb, wvb, kn_hbm, wob, ln2b_hbm, wgb, wub, wdb, xg_hbm,
           out,
           wbuf, wsem, hx, posb, maskb, cosb, sinb, visb, keepb, h, x, act, ctx, qb, kb, vb, vg,
           pb, rcv1, snd2, rcv2, pf, rcvf, obuf, osem, gbuf, ssq, rbuf, acc,
           freq, ln1a, ln2a, ln1b, ln2b, qn, kn, xg, psem,
           lsem, hs, hr, ps, pr, ms, mr, vs, vr, s1, r1, s2, r2, s3, r3, fs, fr):
    d = lax.axis_index('tp')
    core = lax.rem(d, 2)
    part = d + 1 - 2 * core
    cross = lax.rem(d + 2, 4)
    diag = 3 - d
    peers = (part, cross, diag)
    weights = {
        'qa': (wqa,), 'kva': (wka, wva), 'oa': (woa,), 'gua': (wga, wua), 'da': (wda,),
        'qb': (wqb,), 'kvb': (wkb, wvb), 'ob': (wob,), 'gub': (wgb, wub), 'db': (wdb,),
    }

    def cols(index):
        return pl.ds(pl.multiple_of(index * NC, NC), NC)

    def start_segment(name, first, m):
        slot = lax.rem(m, SP)
        i = m - first
        refs = weights[name]
        kind = name[:-1]
        if kind == 'q':
            for half in range(2):
                pltpu.make_async_copy(refs[0].at[:, cols(2 * i + half)], wbuf.at[slot, half], wsem.at[slot, half]).start()
        elif kind == 'kv':
            for half in range(2):
                pltpu.make_async_copy(refs[half], wbuf.at[slot, half], wsem.at[slot, half]).start()
        elif kind == 'gu':
            for half in range(2):
                pltpu.make_async_copy(refs[half].at[:, cols(i)], wbuf.at[slot, half], wsem.at[slot, half]).start()
        elif kind == 'd':
            for half in range(2):
                pltpu.make_async_copy(refs[0].at[:, cols(i + 8 * half)], wbuf.at[slot, half, pl.ds(0, FF)], wsem.at[slot, half]).start()
        else:
            for half in range(2):
                for sub in range(4):
                    pltpu.make_async_copy(refs[0].at[:, cols(4 * i + sub + 8 * half)],
                                          wbuf.at[slot, half, pl.ds(sub * WO_ROWS, WO_ROWS)], wsem.at[slot, half]).start()

    def issue(m, low, high):
        for name, first, count in SEGMENTS:
            if first >= high or first + count <= low:
                continue
            if first <= low and high <= first + count:
                start_segment(name, first, m)
            else:
                @pl.when(jnp.logical_and(m >= first, m < first + count))
                def _():
                    start_segment(name, first, m)

    def refill(m, low, high):
        if low + SP < TOTAL:
            issue(m + SP, low + SP, high + SP)

    def arrive(m, rows=D):
        slot = lax.rem(m, SP)
        for half in range(2):
            dst = wbuf.at[slot, half, pl.ds(0, rows)]
            pltpu.make_async_copy(dst, dst, wsem.at[slot, half]).wait()
        return slot

    def remote(src, dst, send, recv, to):
        return pltpu.make_async_remote_copy(src_ref=src, dst_ref=dst, send_sem=send, recv_sem=recv,
                                            device_id={'tp': to}, device_id_type=MESH)

    own_rows = pltpu.make_async_copy(hid.at[0], hx.at[d], lsem.at[0])
    own_rows.start()
    own_pos = pltpu.make_async_copy(pos, posb.at[d], lsem.at[1])
    own_pos.start()
    own_mask = pltpu.make_async_copy(tmask.at[0], maskb.at[d], lsem.at[2])
    own_mask.start()
    own_vis = pltpu.make_async_copy(vis.at[0], vg.at[d], lsem.at[3])
    own_vis.start()
    small = [pltpu.make_async_copy(src, dst, psem.at[n]) for n, (src, dst) in enumerate((
        (freq_hbm, freq), (ln1a_hbm, ln1a), (ln2a_hbm, ln2a), (ln1b_hbm, ln1b), (ln2b_hbm, ln2b),
        (qn_hbm, qn), (kn_hbm, kn), (xg_hbm, xg)))]
    barrier = pltpu.get_barrier_semaphore()
    for peer in peers:
        pl.semaphore_signal(barrier, inc=1, device_id={'tp': peer}, device_id_type=MESH)
    issue(0, 0, 1)
    for copy in small:
        copy.start()
    for m in range(1, 4):
        issue(m, m, m + 1)
    own_rows.wait()
    own_pos.wait()
    own_mask.wait()
    pl.semaphore_wait(barrier, 3)

    def half_cols(n):
        return pl.ds(pl.multiple_of(n * (D // 2), D // 2), D // 2)

    def hid_cross(block, n):
        piece = hx.at[block, :, half_cols(n)]
        return remote(piece, piece, hs.at[1 + n], hr.at[1 + n], cross)

    def hid_relay(block, n):
        piece = hx.at[block, :, half_cols(n)]
        return remote(piece, piece, hs.at[5 + n], hr.at[5 + n], part)

    def vis_half(block, n, index, to):
        rows = pl.ds(n * (VB // 2), VB // 2)
        return remote(vg.at[block, rows], vg.at[block, rows], vs.at[index], vr.at[index], to)

    first_sends = [hid_cross(d, n) for n in range(2)] + [remote(hx.at[d], hx.at[d], hs.at[0], hr.at[0], part)]
    for k, peer in enumerate(peers):
        first_sends.append(remote(posb.at[d], posb.at[d], ps.at[k], pr.at[k], peer))
        first_sends.append(remote(maskb.at[d], maskb.at[d], ms.at[k], mr.at[k], peer))
    for copy in first_sends:
        copy.start()
    for m in range(4, SP):
        issue(m, m, m + 1)
    vis_part = remote(vg.at[d], vg.at[d], vs.at[0], vr.at[0], part)

    for k, peer in enumerate(peers):
        remote(posb.at[peer], posb.at[peer], ps.at[k], pr.at[k], peer).wait_recv()
        remote(maskb.at[peer], maskb.at[peer], ms.at[k], mr.at[k], peer).wait_recv()

    for copy in small:
        copy.wait()

    sign = jnp.where(lax.broadcasted_iota(jnp.int32, (TB, HD), 1) < HD // 2, -1.0, 1.0)
    eye = lax.broadcasted_iota(jnp.int32, (TB, TB), 0) == lax.broadcasted_iota(jnp.int32, (TB, TB), 1)
    freqs = freq[...]

    def as_column(row):
        return jnp.sum(jnp.where(eye, jnp.broadcast_to(row, (TB, TB)), 0.0), axis=1, keepdims=True)

    for block in range(4):
        rows = pl.ds(block * TB, TB)
        angles = as_column(posb[block].astype(F32)) * freqs
        cosb[rows, :] = jnp.cos(angles)
        sinb[rows, :] = jnp.sin(angles) * sign
        seen = (maskb[block] > 0).astype(F32)
        for tile in range(4):
            visb[rows, tile * (V // 4):(tile + 1) * (V // 4)] = jnp.broadcast_to(as_column(seen[tile:tile + 1]), (TB, V // 4))
        keepb[rows, :] = jnp.broadcast_to(as_column(jnp.max(seen, axis=0, keepdims=True)), (TB, HD))

    for k, gain in enumerate((ln1a, ln2a, ln1b, ln2b)):
        for c in range(D // NC):
            gbuf[k, c] = gain[pl.ds(c * NC, NC)].astype(F32).reshape(1, NC)

    def take(c, value, gain):
        v = value.astype(F32)
        x[:, cols(c)] = (v * gbuf[gain, c]).astype(BF16)
        ssq[...] += v * v

    def row_scale():
        scale = lax.rsqrt(jnp.sum(ssq[...], axis=1, keepdims=True) * (1.0 / D) + NORM_EPS)
        rbuf[...] = jnp.broadcast_to(scale, (T, HD))

    ssq[...] = jnp.zeros((T, NC), F32)
    for e in range(3):
        for half in range(2):
            acc[e, half] = jnp.zeros((T, NC), F32)
        arrive(e)
    for n in range(2):
        hid_cross(cross, n).wait_recv()
        hid_relay(cross, n).start()
    own_vis.wait()
    vis_part.start()
    vis_half(d, 0, 1, cross).start()
    remote(hx.at[part], hx.at[part], hs.at[0], hr.at[0], part).wait_recv()

    def first_stage(n, carry):
        hid_relay(diag, n).wait_recv()
        for k in range(8):
            c = 8 * n + k
            h[c] = hx[:, :, cols(c)].reshape(T, NC)
            take(c, h[c], 0)
        x_part = x[:, half_cols(n)]
        for e in range(3):
            for half in range(2):
                acc[e, half] += dot(x_part, wbuf[e, half, half_cols(n)])
        return carry

    lax.fori_loop(0, 2, first_stage, 0)
    row_scale()

    def head_norm(v, gain):
        scale = lax.rsqrt(jnp.mean(v * v, axis=1, keepdims=True) + NORM_EPS)
        return v * scale * gain[...].astype(F32).reshape(1, HD)

    def rope(v):
        return v * cosb[...] + pltpu.roll(v, HD // 2, 1) * sinb[...]

    def attend(keys, mask):
        for g in range(KV):
            q = qb[pl.ds(g * REP, REP)].reshape(REP * T, HD)
            scores = dot_t(q, kb[g, pl.ds(0, keys)]) * (HD ** -0.5)
            scores = jnp.where(mask, scores, MASK_VALUE)
            top = jnp.max(scores, axis=1, keepdims=True)
            e = jnp.exp(scores - top)
            p = (e / jnp.sum(e, axis=1, keepdims=True)).astype(BF16)
            o = dot(p, vb[g, pl.ds(0, keys)]).astype(BF16)
            for r in range(REP):
                head = g * REP + r
                ctx[:, head * HD:(head + 1) * HD] = o[r * T:(r + 1) * T]

    def spread(parity, partials, update, gain, first, count, between=None):
        def hop1(i):
            return remote(pb.at[1 - core, i], rcv1.at[i], s1.at[i], r1.at[i], part)

        def hop2(i):
            return remote(snd2.at[i], rcv2.at[parity, i], s2.at[parity, i], r2.at[parity, i], cross)

        def hop3(half, i):
            return remote(h.at[half * 8 + i], h.at[half * 8 + i], s3.at[i], r3.at[i], part)

        def fold(i):
            hop1(i).wait_recv()
            snd2[i] = (pb[core, i].astype(F32) + rcv1[i].astype(F32)).astype(BF16)
            hop2(i).start()

        def step(j, carry):
            for n, (low, high) in enumerate(partials(j)):
                i = 2 * j + n
                pb[0, i] = low.astype(BF16)
                pb[1, i] = high.astype(BF16)
                hop1(i).start()

            @pl.when(j >= 1)
            def _():
                fold(2 * j - 2)
                fold(2 * j - 1)
            return carry

        lax.fori_loop(0, 4, step, 0)
        fold(6)
        fold(7)
        if between is not None:
            between()

        def final(i):
            hop2(i).wait_recv()
            total = snd2[i].astype(F32) + rcv2[parity, i].astype(F32)
            mine = core * 8 + i
            value = (h[mine].astype(F32) + update(total)).astype(BF16)
            h[mine] = value
            hop3(core, i).start()
            take(mine, value, gain)

        ssq[...] = jnp.zeros((T, NC), F32)
        for e in range(count):
            for half in range(2):
                acc[e, half] = jnp.zeros((T, NC), F32)
        final(0)
        final(1)

        def stage(n, carry):
            @pl.when(n < 3)
            def _():
                final(2 * n + 2)
                final(2 * n + 3)

            @pl.when(n == 0)
            def _():
                for e in range(count):
                    arrive(first + e)
            for k in range(2):
                i = 2 * n + k
                theirs = (1 - core) * 8 + i
                hop3(1 - core, i).wait_recv()
                take(theirs, h[theirs], gain)
            low = pl.ds(pl.multiple_of(n * 2 * NC, 2 * NC), 2 * NC)
            high = pl.ds(pl.multiple_of(n * 2 * NC + D // 2, 2 * NC), 2 * NC)
            x_low, x_high = x[:, low], x[:, high]
            for e in range(count):
                slot = (first + e) % SP
                for half in range(2):
                    acc[e, half] += dot(x_low, wbuf[slot, half, low]) + dot(x_high, wbuf[slot, half, high])
            return carry

        lax.fori_loop(0, 4, stage, 0)
        row_scale()

        def finish(i, carry):
            hop3(core, i).wait_send()
            hop1(i).wait_send()
            hop2(i).wait_send()
            return carry

        lax.fori_loop(0, 8, finish, 0)

    def wo_partials(base):
        def partials(j):
            m = base + j // 2
            slot = lax.rem(m, SP)

            @pl.when(lax.rem(j, 2) == 0)
            def _():
                arrive(m)
            out = []
            for n in range(2):
                rows = pl.ds(pl.multiple_of((lax.rem(j, 2) * 2 + n) * WO_ROWS, WO_ROWS), WO_ROWS)
                out.append((dot(ctx[...], wbuf[slot, 0, rows]), dot(ctx[...], wbuf[slot, 1, rows])))

            @pl.when(lax.rem(j, 2) == 1)
            def _():
                refill(m, base, base + 2)
            return out
        return partials

    def wd_partials(base, count=2):
        def partials(j):
            slots = [arrive(base + count * j + n, FF) for n in range(count)]
            out = []
            for slot in slots:
                rows = pl.ds(0, FF)
                out.append((dot(act[...], wbuf[slot, 0, rows]), dot(act[...], wbuf[slot, 1, rows])))
            for n in range(count):
                refill(base + count * j + n, base, base + 8)
            return out
        return partials

    def mlp_up(base):
        def activate(i, gate, up):
            gate = gate * rbuf[:, 0:1]
            act[:, cols(i)] = (gate * jax.nn.sigmoid(gate) * (up * rbuf[:, 0:1])).astype(BF16)

        for e in range(EARLY):
            activate(e, acc[e, 0], acc[e, 1])
            refill(base + e, base + e, base + e + 1)

        def step(i, carry):
            slots = [arrive(base + 2 * i + n) for n in range(2)]
            for n, slot in enumerate(slots):
                activate(2 * i + n, dot(x[...], wbuf[slot, 0]), dot(x[...], wbuf[slot, 1]))
            for n in range(2):
                refill(base + 2 * i + n, base + EARLY, base + 14)
            return carry
        lax.fori_loop(EARLY // 2, 7, step, 0)

    def queries(products, finish):
        for n, q in enumerate(products):
            q = q * rbuf[:, 0:1]
            for sub in range(2):
                qb[2 * n + sub] = finish(q[:, sub * HD:(sub + 1) * HD]).astype(BF16)

    queries([acc[e, half] for e in range(2) for half in range(2)], rope)
    keys, vals = [acc[2, half] * rbuf[:, 0:1] for half in range(2)]
    for g in range(KV):
        kb[g, pl.ds(0, T)] = rope(keys[:, g * HD:(g + 1) * HD]).astype(BF16)
        vb[g, pl.ds(0, T)] = vals[:, g * HD:(g + 1) * HD].astype(BF16)
    for m in range(3):
        refill(m, m, m + 1)
    query_at = lax.rem(lax.broadcasted_iota(jnp.int32, (REP * T, T), 0), T)
    attend(T, query_at >= lax.broadcasted_iota(jnp.int32, (REP * T, T), 1))

    def vision_send():
        vis_half(d, 1, 2, cross).start()

    spread(0, wo_partials(BASE['oa']), lambda total: total, 1, BASE['gua'], EARLY, vision_send)
    mlp_up(BASE['gua'])
    down_a = wd_partials(BASE['da'])

    def down_and_forward(j):
        @pl.when(j == 1)
        def _():
            for n in range(2):
                vis_half(cross, n, 1 + n, cross).wait_recv()
                vis_half(cross, n, 3 + n, part).start()
        return down_a(j)

    def vision_heads():
        remote(vg.at[part], vg.at[part], vs.at[0], vr.at[0], part).wait_recv()
        for n in range(2):
            vis_half(diag, n, 3 + n, part).wait_recv()
        slot = arrive(BASE['kvb'])

        def kv_step(n, carry):
            rows = pl.ds(pl.multiple_of(n * 2 * VB, 2 * VB), 2 * VB)
            lhs = vg[pl.ds(2 * n, 2)].reshape(2 * VB, D)
            keys = dot(lhs, wbuf[slot, 0])
            vals = dot(lhs, wbuf[slot, 1])
            for g in range(KV):
                kb[g, rows] = head_norm(keys[:, g * HD:(g + 1) * HD], kn).astype(BF16)
                vb[g, rows] = vals[:, g * HD:(g + 1) * HD].astype(BF16)
            return carry

        lax.fori_loop(0, 2, kv_step, 0)
        refill(BASE['kvb'], BASE['kvb'], BASE['kvb'] + 1)

    spread(1, down_and_forward, lambda total: total, 2, BASE['qb'], 2, vision_heads)

    queries([acc[e, half] for e in range(2) for half in range(2)], lambda q: head_norm(q, qn))
    for i in range(2):
        refill(BASE['qb'] + i, BASE['qb'] + i, BASE['qb'] + i + 1)
    attend(V, jnp.concatenate([visb[...]] * REP, axis=0) > 0.0)
    gate0 = jnp.tanh(jnp.full((T, 1), xg[0], F32)) * keepb[:, 0:1]
    spread(2, wo_partials(BASE['ob']), lambda total: gate0 * total, 3, BASE['gub'], EARLY)
    mlp_up(BASE['gub'])

    own = pl.ds(pl.multiple_of(d * TB, TB), TB)
    gate1 = jnp.tanh(jnp.full((TB, 1), xg[1], F32)) * keepb[own, 0:1]
    down = wd_partials(BASE['db'], 1)

    def last_step(j, carry):
        for half, value in enumerate(down(j)[0]):
            pf[j, :, half] = value.astype(BF16).reshape(4, TB, NC)
        for k, peer in enumerate(peers):
            remote(pf.at[j, peer], rcvf.at[j, k], fs.at[j, k], fr.at[j, k], peer).start()
        return carry

    lax.fori_loop(0, 8, last_step, 0)

    def last_sum(i, carry):
        for k, peer in enumerate(peers):
            remote(pf.at[i, peer], rcvf.at[i, k], fs.at[i, k], fr.at[i, k], peer).wait_recv()
        for half in range(2):
            total = pf[i, d, half].astype(F32)
            for k in range(3):
                total = total + rcvf[i, k, half].astype(F32)
            chunk = i + 8 * half
            obuf[:, cols(chunk)] = (h[chunk, own].astype(F32) + gate1 * total).astype(BF16)
            pltpu.make_async_copy(obuf.at[:, cols(chunk)], out.at[0, :, cols(chunk)], osem.at[i, half]).start()
        return carry

    lax.fori_loop(0, 8, last_sum, 0)

    for copy in first_sends:
        copy.wait_send()
    vis_part.wait_send()
    for n in range(2):
        hid_relay(cross, n).wait_send()
        vis_half(d, n, 1 + n, cross).wait_send()
        vis_half(cross, n, 3 + n, part).wait_send()

    def drain(j, carry):
        for half in range(2):
            piece = cols(j + 8 * half)
            pltpu.make_async_copy(obuf.at[:, piece], out.at[0, :, piece], osem.at[j, half]).wait()
        for k, peer in enumerate(peers):
            remote(pf.at[j, peer], rcvf.at[j, k], fs.at[j, k], fr.at[j, k], peer).wait_send()
        return carry

    lax.fori_loop(0, 8, drain, 0)


def solution(mesh):
    act_spec = P('dp', 'tp', None)
    col_spec = P(None, 'tp')
    row_spec = P('tp', None)
    layer_a = (P(), col_spec, col_spec, col_spec, row_spec, P(), col_spec, col_spec, row_spec)
    layer_b = (P(), col_spec, P(), col_spec, col_spec, P(), row_spec, P(), col_spec, col_spec, row_spec, P())
    in_specs = (act_spec, act_spec, P('dp', 'tp'), act_spec) + layer_a + layer_b
    table = rope_table(HD)

    hbm = pl.BlockSpec(memory_space=pl.ANY)
    dma = pltpu.SemaphoreType.DMA
    scratch = [
        pltpu.VMEM((SP, 2, D, NC), BF16), dma((SP, 2)),
        pltpu.VMEM((4, TB, D), BF16),
        pltpu.VMEM((4, 1, TB), jnp.int32),
        pltpu.VMEM((4, 4, TB), jnp.int32),
        pltpu.VMEM((T, HD), F32), pltpu.VMEM((T, HD), F32),
        pltpu.VMEM((T, V), F32), pltpu.VMEM((T, HD), F32),
        pltpu.VMEM((D // NC, T, NC), BF16),
        pltpu.VMEM((T, D), BF16),
        pltpu.VMEM((T, FF), BF16),
        pltpu.VMEM((T, WO_ROWS), BF16),
        pltpu.VMEM((KV * REP, T, HD), BF16),
        pltpu.VMEM((KV, V, HD), BF16), pltpu.VMEM((KV, V, HD), BF16),
        pltpu.VMEM((4, VB, D), BF16),
        pltpu.VMEM((2, 8, T, NC), BF16),
        pltpu.VMEM((8, T, NC), BF16),
        pltpu.VMEM((8, T, NC), BF16),
        pltpu.VMEM((3, 8, T, NC), BF16),
        pltpu.VMEM((8, 4, 2, TB, NC), BF16),
        pltpu.VMEM((8, 3, 2, TB, NC), BF16),
        pltpu.VMEM((TB, D), BF16), dma((8, 2)),
        pltpu.VMEM((4, D // NC, 1, NC), F32), pltpu.VMEM((T, NC), F32), pltpu.VMEM((T, HD), F32),
        pltpu.VMEM((EARLY, 2, T, NC), F32),
        pltpu.VMEM((1, HD), F32), pltpu.VMEM((D,), BF16), pltpu.VMEM((D,), BF16), pltpu.VMEM((D,), BF16), pltpu.VMEM((D,), BF16),
        pltpu.VMEM((HD,), BF16), pltpu.VMEM((HD,), BF16), pltpu.SMEM((2,), F32), dma((8,)),
        dma((4,)),
        dma((9,)), dma((9,)), dma((3,)), dma((3,)), dma((3,)), dma((3,)),
        dma((5,)), dma((5,)),
        dma((8,)), dma((8,)), dma((3, 8)), dma((3, 8)), dma((8,)), dma((8,)),
        dma((8, 3)), dma((8, 3)),
    ]

    def body(hidden, vision, positions, tile_mask, *params):
        freqs = jnp.asarray(np.concatenate([table, table])[None])
        specs = [hbm] * (5 + len(params))
        return pl.pallas_call(
            kernel,
            out_shape=jax.ShapeDtypeStruct(hidden.shape, BF16),
            in_specs=specs,
            out_specs=hbm,
            scratch_shapes=scratch,
            compiler_params=pltpu.CompilerParams(
                collective_id=0, has_side_effects=True, vmem_limit_bytes=67043328),
            cost_estimate=pl.CostEstimate(flops=2 * 64 * 109051904, bytes_accessed=218103808, transcendentals=0),
            name='layers',
        )(hidden, vision, positions, jnp.swapaxes(tile_mask, 1, 2), freqs, *params)

    return jax.shard_map(body, mesh=mesh, in_specs=in_specs, out_specs=act_spec, check_vma=False)
```
